128 devices in a mesh: dp: 1, row: 2 (over core), col: 64 (over z, y, x).
Axes of the slice: x: 4, y: 4, z: 4, core: 2. Of those that a mesh axis runs over, the one named last changes fastest.
Arguments:
- x: bfloat16 [2, 128, 128, 2048], P(None, ('dp', 'row', 'col'))
- idx: int32 [2, 128, 128, 8], P(None, ('dp', 'row', 'col'))
- gates: float32 [2, 128, 128, 8], P(None, ('dp', 'row', 'col'))
- wq: bfloat16 [2048, 4096], replicated
- wk: bfloat16 [2048, 4096], replicated
- wv: bfloat16 [2048, 4096], replicated
- wo: bfloat16 [4096, 2048], replicated
- gattn: float32 [2048], replicated
- gmoe: float32 [2048], replicated
- w1: bfloat16 [128, 2048, 768], P(('row', 'col'))
- w3: bfloat16 [128, 2048, 768], P(('row', 'col'))
- w2: bfloat16 [128, 768, 2048], P(('row', 'col'))
Outputs:
- output: bfloat16 [2, 128, 128, 2048], P(None, ('dp', 'row', 'col'))
All inputs are finite; a program needn't handle non-finite values.
Results may differ from the reference program's by a relative error of at most 0.0107599.
Values are sent between devices in bfloat16 or wider.
A program may use at most 1 GiB of HBM per device.

```python
import jax
import jax.numpy as jnp
from jax import lax

D = 2048
HEADS = 32
HEAD = 128
EXPERTS = 128
TOP = 8
FF = 768
TOKENS = 128
SEQ = 128
GROUP = 128

CAP = ((TOP * ((2 * TOKENS + EXPERTS - 1) // EXPERTS) + 7) // 8) * 8
NTOK = GROUP * TOKENS
NSEQ = NTOK // SEQ


def draw_routing(key):
    k1, k2, k3 = jax.random.split(key, 3)
    k1 = jax.random.fold_in(k1, 7919)
    k2 = jax.random.fold_in(k2, 7919)
    offset = jax.random.randint(k1, (), 0, EXPERTS)
    ranks = jax.vmap(lambda kk: jax.random.permutation(kk, TOKENS))(jax.random.split(k2, GROUP))
    half = TOKENS // 2
    quarter = EXPERTS // 4
    r = jnp.where(ranks < half, (ranks * quarter) // half, quarter + ((ranks - half) * (EXPERTS - quarter)) // half)
    pos = (offset + r[:, :, None] - jnp.arange(TOP)[None, None, :]) % EXPERTS
    idx = pos.reshape(NSEQ, SEQ, TOP).astype(jnp.int32)
    gates = jax.nn.softmax(jax.random.normal(k3, (NSEQ, SEQ, TOP), jnp.float32), axis=-1)
    return idx, gates


def setup_inputs(seed: int = 0, part: int = 0) -> dict:
    key = jax.random.key(seed)
    kw = jax.random.split(key, 10)
    kp = jax.random.split(jax.random.fold_in(key, part), 4)
    hd = HEADS * HEAD
    base = jax.random.normal(kp[0], (2, NSEQ, SEQ, D), jnp.float32)
    shift = 0.8 * jax.random.normal(kp[1], (2, NSEQ, 1, D), jnp.float32)
    x = (base + shift).astype(jnp.bfloat16)
    ia, ga = draw_routing(kp[2])
    ib, gb = draw_routing(kp[3])
    idx = jnp.stack([ia, ib])
    gates = jnp.stack([ga, gb])
    wq = (jax.random.normal(kw[0], (D, hd), jnp.float32) * D ** -0.5).astype(jnp.bfloat16)
    wk = (jax.random.normal(kw[1], (D, hd), jnp.float32) * D ** -0.5).astype(jnp.bfloat16)
    wv = (jax.random.normal(kw[2], (D, hd), jnp.float32) * D ** -0.5).astype(jnp.bfloat16)
    wo = (jax.random.normal(kw[3], (hd, D), jnp.float32) * hd ** -0.5).astype(jnp.bfloat16)
    gattn = 1.0 + 0.3 * jax.random.normal(kw[4], (D,), jnp.float32)
    gmoe = 1.0 + 0.3 * jax.random.normal(kw[5], (D,), jnp.float32)
    w1 = (jax.random.normal(kw[6], (EXPERTS, D, FF), jnp.float32) * D ** -0.5).astype(jnp.bfloat16)
    w3 = (jax.random.normal(kw[7], (EXPERTS, D, FF), jnp.float32) * D ** -0.5).astype(jnp.bfloat16)
    w2 = (jax.random.normal(kw[8], (EXPERTS, FF, D), jnp.float32) * 2.0 * FF ** -0.5).astype(jnp.bfloat16)
    return {"x": x, "idx": idx, "gates": gates, "wq": wq, "wk": wk, "wv": wv, "wo": wo, "gattn": gattn, "gmoe": gmoe, "w1": w1, "w3": w3, "w2": w2}


def rms(v, g):
    vf = v.astype(jnp.float32)
    return (vf * lax.rsqrt(jnp.mean(vf * vf, axis=-1, keepdims=True) + 1e-6) * g).astype(jnp.bfloat16)


def attention(x, wq, wk, wv, wo, gattn):
    u = rms(x, gattn)

    def proj(w):
        a = jnp.dot(u, w, preferred_element_type=jnp.float32).astype(jnp.bfloat16)
        return a.reshape(NSEQ, SEQ, HEADS, HEAD).transpose(2, 0, 1, 3)

    q, k, v = proj(wq), proj(wk), proj(wv)
    causal = jnp.arange(SEQ)[:, None] >= jnp.arange(SEQ)[None, :]

    def one_head(qkv):
        qh, kh, vh = qkv
        s = jnp.einsum("cre,cle->crl", qh.astype(jnp.float32), kh.astype(jnp.float32)) * HEAD ** -0.5
        s = jnp.where(causal[None], s, -1e30)
        p = jax.nn.softmax(s, axis=-1).astype(jnp.bfloat16)
        o = jnp.einsum("crl,cle->cre", p.astype(jnp.float32), vh.astype(jnp.float32))
        return o.astype(jnp.bfloat16)

    o = lax.map(one_head, (q, k, v))
    o = o.transpose(1, 2, 0, 3).reshape(NTOK, HEADS * HEAD)
    a = jnp.dot(o, wo, preferred_element_type=jnp.float32)
    return (x.astype(jnp.float32) + a).astype(jnp.bfloat16)


def moe(h, idx, gates, w1, w3, w2, gmoe):
    z = rms(h, gmoe)
    zpad = jnp.concatenate([z, jnp.zeros((1, D), jnp.bfloat16)], axis=0)
    flat = idx.reshape(-1)
    gflat = gates.reshape(-1)
    order = jnp.argsort(flat, stable=True)
    counts = jnp.zeros((EXPERTS,), jnp.int32).at[flat].add(1)
    starts = jnp.cumsum(counts) - counts
    width = GROUP * CAP

    def step(acc, per_expert):
        a1, a3, a2, st, ct = per_expert
        slot = st + jnp.arange(width)
        valid = slot < st + ct
        pair = order[jnp.minimum(slot, NTOK * TOP - 1)]
        tok = jnp.where(valid, pair // TOP, NTOK)
        gate = jnp.where(valid, gflat[pair], 0.0)
        rows = zpad[tok]
        h1 = jnp.dot(rows, a1, preferred_element_type=jnp.float32)
        h3 = jnp.dot(rows, a3, preferred_element_type=jnp.float32)
        act = (jax.nn.silu(h1) * h3).astype(jnp.bfloat16)
        out = jnp.dot(act, a2, preferred_element_type=jnp.float32).astype(jnp.bfloat16)
        acc = acc.at[tok].add(gate[:, None] * out.astype(jnp.float32), mode="drop")
        return acc, None

    acc, _ = lax.scan(step, jnp.zeros((NTOK, D), jnp.float32), (w1, w3, w2, starts, counts))
    return (h.astype(jnp.float32) + acc).astype(jnp.bfloat16)


def reference(x, idx, gates, wq, wk, wv, wo, gattn, gmoe, w1, w3, w2):
    ys = []
    for m in range(2):
        h = attention(x[m].reshape(NTOK, D), wq, wk, wv, wo, gattn)
        y = moe(h, idx[m].reshape(NTOK, TOP), gates[m].reshape(NTOK, TOP), w1, w3, w2, gmoe)
        ys.append(y.reshape(NSEQ, SEQ, D))
    return jnp.stack(ys)
```

```python
import functools

import jax
import jax.numpy as jnp
from jax import lax
from jax.experimental import pallas as pl
from jax.experimental.pallas import tpu as pltpu
from jax.sharding import PartitionSpec as P

HEAD = 128
VMEM_LIMIT = 67_000_000
MESH = pl.DeviceIdType.MESH
BF = jnp.bfloat16
F32 = jnp.float32
RING = 4
CORES = 2
COEF = {"z": 16, "y": 4, "x": 1}
PARTS = (("x", "y", "z"), ("y", "z", "x"), ("z", "x", "y"))
TILES = CORES * RING


def widths(d):
    lanes = d // 128
    base = lanes // 3
    return (base * 128, base * 128, (lanes - 2 * base) * 128)


class Sems:
    def __init__(self):
        self.n = 0

    def take(self, k=1):
        self.n += k
        return self.n - k


def moe_kernel(dims, nsem, z_hbm, h_ref, idx_ref, gate_ref, w1_hbm, w3_hbm, w2_hbm,
               y_ref, *rest):
    T, D, FF, CAP, TOP, COLS = dims
    it = iter(rest)
    recv = [next(it) for _ in range(3)]
    outp = [next(it) for _ in range(3)]
    ptr = [next(it) for _ in range(3)]
    r1 = [next(it) for _ in range(3)]
    r1t = [next(it) for _ in range(3)]
    r2 = [next(it) for _ in range(3)]
    r2t = [next(it) for _ in range(3)]
    ag = [next(it) for _ in range(3)]
    sbuf = [next(it) for _ in range(3)]
    mi = next(it)
    mg = next(it)
    lst = [next(it) for _ in range(3)]
    w1, w3, w2, xbuf, obuf = (next(it) for _ in range(5))
    stage = next(it)
    part_acc = [next(it) for _ in range(3)]
    q1 = [next(it) for _ in range(3)]
    q2 = [next(it) for _ in range(3)]
    hbuf = next(it)
    ssem, rsem = next(it), next(it)
    xsem, osem, lsem = next(it), next(it), next(it)

    c = lax.axis_index("row")
    q = lax.axis_index("col")
    pos = {"z": q // 16, "y": (q // 4) % 4, "x": q % 4}
    S, R = Sems(), Sems()
    pending = {}
    offs = (0, COLS[0], COLS[0] + COLS[1])

    def rel(v, s):
        return (v + s + RING) % RING

    def nb(dim, s, core=None):
        v = dict(pos)
        v[dim] = rel(v[dim], s)
        return {"row": c if core is None else core, "col": v["z"] * 16 + v["y"] * 4 + v["x"]}

    def send(src, dst, dev, si, ri):
        cp = pltpu.make_async_remote_copy(src_ref=src, dst_ref=dst, send_sem=ssem.at[si], recv_sem=rsem.at[ri],
                                          device_id=dev, device_id_type=MESH)
        cp.start()
        pending[id(cp)] = cp
        return cp

    def wait_in(ref, ri, dev):
        pltpu.make_async_remote_copy(src_ref=ref, dst_ref=ref, send_sem=ssem.at[0], recv_sem=rsem.at[ri],
                                     device_id=dev, device_id_type=MESH).wait_recv()

    barrier = pltpu.get_barrier_semaphore()
    friends = [nb(d, s, core) for d in "xyz" for s in (1, -1) for core in (c, 1 - c)]
    friends.append({"row": 1 - c, "col": q})
    for f in friends:
        pl.semaphore_signal(barrier, inc=1, device_id=f, device_id_type=MESH)
    wload = []
    for i, (a, b) in enumerate(((w1_hbm, w1), (w3_hbm, w3), (w2_hbm, w2))):
        cp = pltpu.make_async_copy(a.at[0], b, lsem.at[i])
        cp.start()
        wload.append(cp)
    own = {}
    for m in range(2):
        for p, (d1, d2, d3) in enumerate(PARTS):
            cp = pltpu.make_async_copy(z_hbm.at[m, :, pl.ds(offs[p], COLS[p])], ag[p].at[m, pos[d2], pos[d1]],
                                       lsem.at[3 + m * 3 + p])
            cp.start()
            own[m, p] = cp
    for p, (d1, d2, d3) in enumerate(PARTS):
        mi[p, pos[d2], pos[d1]] = idx_ref[...]
        mg[p, pos[d1]] = gate_ref[...]
    pl.semaphore_wait(barrier, len(friends))

    def ring1(dim, block):
        me = pos[dim]
        a = send(block(me, None), block(me, None), nb(dim, 1), S.take(), R.take())
        b = send(block(me, None), block(me, None), nb(dim, -1), S.take(), R.take())
        return a, b

    def ring2(dim, block, ab):
        me = pos[dim]
        ab[0].wait_recv()
        a = send(block(rel(me, -1), 0), block(rel(me, -1), 0), nb(dim, 1), S.take(), R.take())
        ab[1].wait_recv()
        b = send(block(rel(me, 1), 1), block(rel(me, 1), 1), nb(dim, -1), S.take(), R.take())
        return a, b

    def ring3(ab):
        ab[0].wait_recv()
        ab[1].wait_recv()

    def blk1(m, p):
        d2 = PARTS[p][1]

        def f(i, half):
            if half is None:
                return ag[p].at[m, pos[d2], i]
            return ag[p].at[m, pos[d2], i, pl.ds(half * (T // 2), T // 2)]
        return f

    def blk2(m, p):
        def f(i, half):
            if half is None:
                return ag[p].at[m, i]
            return ag[p].at[m, i, pl.ds(half * 2, 2)]
        return f

    def mi1(p):
        d2 = PARTS[p][1]

        def f(i, half):
            if half is None:
                return mi.at[p, pos[d2], i]
            return mi.at[p, pos[d2], i, half]
        return f

    def mg1(p):
        def f(i, half):
            if half is None:
                return mg.at[p, i]
            return mg.at[p, i, half]
        return f

    def mi2(p):
        def f(i, half):
            if half is None:
                return mi.at[p, i]
            return mi.at[p, i, pl.ds(half * 2, 2)]
        return f

    P3 = range(3)
    mim = [ring1(PARTS[p][0], mi1(p)) for p in P3]
    mgm = [ring1(PARTS[p][0], mg1(p)) for p in P3]
    s1 = {}
    for m in range(2):
        for p in P3:
            own[m, p].wait()
            s1[m, p] = ring1(PARTS[p][0], blk1(m, p))
    mim = [ring2(PARTS[p][0], mi1(p), mim[p]) for p in P3]
    mgm = [ring2(PARTS[p][0], mg1(p), mgm[p]) for p in P3]
    for m in range(2):
        for p in P3:
            s1[m, p] = ring2(PARTS[p][0], blk1(m, p), s1[m, p])
    for p in P3:
        ring3(mim[p])
        ring3(mgm[p])
    mim = [ring1(PARTS[p][1], mi2(p)) for p in P3]
    for m in range(2):
        for p in P3:
            ring3(s1[m, p])
            s1[m, p] = ring1(PARTS[p][1], blk2(m, p))
    mim = [ring2(PARTS[p][1], mi2(p), mim[p]) for p in P3]
    for m in range(2):
        for p in P3:
            s1[m, p] = ring2(PARTS[p][1], blk2(m, p), s1[m, p])
    for p in P3:
        ring3(mim[p])

    before = (lax.broadcasted_iota(jnp.int32, (T, T), 0) < lax.broadcasted_iota(jnp.int32, (T, T), 1)).astype(BF)

    def hits(rows, e, idx, gate):
        hit = jnp.zeros((rows, T), F32)
        g = jnp.zeros((rows, T), F32)
        for j in range(TOP):
            eq = jnp.broadcast_to(idx[j:j + 1, :], (rows, T)) == e
            hit = jnp.where(eq, 1.0, hit)
            if gate is not None:
                g = jnp.where(eq, jnp.broadcast_to(gate[j:j + 1, :], (rows, T)), g)
        return hit, g

    def ranks(hit):
        cum = jnp.dot(hit.astype(BF), before, preferred_element_type=F32)
        return jnp.where(hit > 0.0, cum, -1.0)

    def spread(rank, rows):
        slot = lax.broadcasted_iota(jnp.int32, (rows, CAP, T), 1).astype(F32)
        return jnp.broadcast_to(rank[:, None, :], (rows, CAP, T)) == slot

    def build(m, p):
        d1, d2, d3 = PARTS[p]
        r = lax.broadcasted_iota(jnp.int32, (2 * RING, T), 0)
        e = (r % 2) * 64 + COEF[d3] * ((pos[d3] + r // 2) % RING) + COEF[d2] * pos[d2] + COEF[d1] * pos[d1]

        def table(s, _):
            hit, _g = hits(2 * RING, e, mi[p, s // 4, s % 4, m], None)
            hbuf[s] = hit
            return 0

        lax.fori_loop(0, 16, table, 0)
        rk = ranks(hbuf[...].reshape(16 * 8, T))
        hbuf[...] = rk.reshape(16, 8, T)

        def one(s, _):
            sel = jnp.where(spread(hbuf[s], 8), 1.0, 0.0).reshape(8 * CAP, T).astype(BF)
            rows = jnp.dot(sel, ag[p][m, s // 4, s % 4], preferred_element_type=F32).astype(BF)
            rows = rows.reshape(8, CAP, COLS[p])
            if p == 2:
                sbuf[p][:, s % 4, s // 4] = rows
            else:
                sbuf[p][:, s // 4, s % 4] = rows
            return 0

        lax.fori_loop(0, 16, one, 0)

    def plane(ref, p, core, t):
        if p == 0:
            return ref.at[core, t]
        if p == 1:
            return ref.at[core, :, :, t]
        return ref.at[core, :, t]

    def x_start(p, src, dst, transit):
        dim = PARTS[p][2]
        me = pos[dim]
        st = {}
        st["t"] = (send(src(2, 0), transit.at[0], nb(dim, 1), S.take(), R.take()),
                   send(src(2, 1), transit.at[1], nb(dim, -1), S.take(), R.take()))
        st["l"], st["r"], st["o"], st["d"] = R.take(2), R.take(2), R.take(2), R.take()
        st["s"] = []
        for core in range(2):
            st["s"].append(send(src(1, core), dst(me, c), nb(dim, 1, core), S.take(), st["l"] + c))
            st["s"].append(send(src(3, core), dst(me, c), nb(dim, -1, core), S.take(), st["r"] + c))
        st["s"].append(send(src(0, 1 - c), dst(me, c), {"row": 1 - c, "col": q}, S.take(), st["d"]))
        st["s"].extend(st["t"])
        return st

    def x_forward(p, dst, transit, st):
        dim = PARTS[p][2]
        me = pos[dim]
        st["t"][0].wait_recv()
        send(transit.at[0], dst(rel(me, -1), c), nb(dim, 1, 0), S.take(), st["o"] + c)
        st["t"][1].wait_recv()
        send(transit.at[1], dst(rel(me, 1), c), nb(dim, -1, 1), S.take(), st["o"] + c)

    def x_wait(p, dst, st):
        dim = PARTS[p][2]
        me = pos[dim]
        for core in range(2):
            wait_in(dst(rel(me, -1), core), st["l"] + core, nb(dim, -1, core))
            wait_in(dst(rel(me, 1), core), st["r"] + core, nb(dim, 1, core))
            wait_in(dst(rel(me, 2), core), st["o"] + core, nb(dim, 1, core))
        wait_in(dst(me, 1 - c), st["d"], {"row": 1 - c, "col": q})

    def p_src(m, p):
        return lambda k, core: sbuf[p].at[2 * k + core]

    def p_dst(m, p):
        return lambda d3v, core: plane(recv[p].at[m], p, core, d3v)

    def r_src(m, p):
        return lambda k, core: plane(outp[p].at[m], p, core, rel(pos[PARTS[p][2]], k))

    def r_dst(m, p):
        return lambda d3v, core: r1[p].at[m, d3v, core]

    pst, loc = {}, {}

    def dispatch(m):
        for p in P3:
            ring3(s1[m, p])
            if m == 1:
                for cp in pst[0, p]["s"]:
                    cp.wait_send()
                    del pending[id(cp)]
                loc[0, p].wait()
            build(m, p)
            pst[m, p] = x_start(p, p_src(m, p), p_dst(m, p), ptr[p].at[m])
            cp = pltpu.make_async_copy(sbuf[p].at[c], p_dst(m, p)(pos[PARTS[p][2]], c), lsem.at[9 + m * 3 + p])
            cp.start()
            loc[m, p] = cp

    def p_forward(m):
        for p in P3:
            x_forward(p, p_dst(m, p), ptr[p].at[m], pst[m, p])

    def p_wait(m):
        for p in P3:
            x_wait(p, p_dst(m, p), pst[m, p])
            if m == 1:
                loc[m, p].wait()

    rows_t = RING * RING * CAP

    def xload(m, i, slot):
        return [pltpu.make_async_copy(recv[p].at[m, i // 4, i % 4], xbuf.at[slot, :, :, :, pl.ds(offs[p], COLS[p])],
                                      xsem.at[slot, p]) for p in P3]

    def ostore(m, i, slot):
        return [pltpu.make_async_copy(obuf.at[slot, :, :, :, pl.ds(offs[p], COLS[p])], outp[p].at[m, i // 4, i % 4],
                                      osem.at[slot, p]) for p in P3]

    def expert(m, lo, hi):
        if lo == 0:
            for cp in xload(m, 0, 0):
                cp.start()

        def tile(i, _):
            slot = i % 2

            @pl.when(i + 1 < TILES)
            def _():
                for cp in xload(m, i + 1, (i + 1) % 2):
                    cp.start()

            for cp in xload(m, i, slot):
                cp.wait()

            @pl.when(i >= 2)
            def _():
                for cp in ostore(m, i - 2, slot):
                    cp.wait()

            xt = xbuf[slot].reshape(rows_t, D)
            h1 = jnp.dot(xt, w1[...], preferred_element_type=F32)
            h3 = jnp.dot(xt, w3[...], preferred_element_type=F32)
            act = (jax.nn.silu(h1) * h3).astype(BF)
            o = jnp.dot(act, w2[...], preferred_element_type=F32).astype(BF)
            obuf[slot] = o.reshape(RING, RING, CAP, D)
            for cp in ostore(m, i, slot):
                cp.start()
            return 0

        lax.fori_loop(lo, hi, tile, 0)
        if hi == TILES:
            for i in (TILES - 2, TILES - 1):
                for cp in ostore(m, i, i % 2):
                    cp.wait()

    rst = {}

    def r1_start(m):
        cps = []
        for p in P3:
            rst[m, p] = x_start(p, r_src(m, p), r_dst(m, p), r1t[p].at[m])
            cp = pltpu.make_async_copy(r_src(m, p)(0, c), lst[p], lsem.at[15 + p])
            cp.start()
            cps.append(cp)
        for p in P3:
            cps[p].wait()
            cp = pltpu.make_async_copy(lst[p], r_dst(m, p)(pos[PARTS[p][2]], c), lsem.at[15 + p])
            cp.start()
            cps[p] = cp
        for p in P3:
            cps[p].wait()

    def r1_forward(m):
        for p in P3:
            x_forward(p, r_dst(m, p), r1t[p].at[m], rst[m, p])

    def r1_for(m, p, t):
        return r1[p].at[m, :, :, :, t] if p == 2 else r1[p].at[m, :, :, t]

    def r1_half(m, p, t, half):
        hs = pl.ds(2 * half, 2)
        return r1[p].at[m, hs, :, :, t] if p == 2 else r1[p].at[m, hs, :, t]

    r2st = {}

    def r2_start(m):
        for p in P3:
            x_wait(p, r_dst(m, p), rst[m, p])
            dim = PARTS[p][1]
            me = pos[dim]
            st = {}
            st["t"] = (send(r1_half(m, p, rel(me, 2), 0), r2t[p].at[m, 0], nb(dim, 1), S.take(), R.take()),
                       send(r1_half(m, p, rel(me, 2), 1), r2t[p].at[m, 1], nb(dim, -1), S.take(), R.take()))
            st["n"] = (send(r1_for(m, p, rel(me, 1)), r2[p].at[m, me], nb(dim, 1), S.take(), R.take()),
                       send(r1_for(m, p, rel(me, -1)), r2[p].at[m, me], nb(dim, -1), S.take(), R.take()))
            r2st[m, p] = st

    def r2_forward(m):
        for p in P3:
            dim = PARTS[p][1]
            me = pos[dim]
            st = r2st[m, p]
            st["t"][0].wait_recv()
            a = send(r2t[p].at[m, 0], r2[p].at[m, rel(me, -1), pl.ds(0, 2)], nb(dim, 1), S.take(), R.take())
            st["t"][1].wait_recv()
            b = send(r2t[p].at[m, 1], r2[p].at[m, rel(me, 1), pl.ds(2, 2)], nb(dim, -1), S.take(), R.take())
            st["f"] = (a, b)

    def r2_wait(m, p):
        st = r2st[m, p]
        for cp in st["n"] + st["f"]:
            cp.wait_recv()

    def stage_in(m, p, k, slot):
        d1, d2, d3 = PARTS[p]
        s1v = rel(pos[d1], k)
        cols = pl.ds(0, COLS[p])
        mine = r1[p].at[m, :, :, s1v, pos[d2]] if p == 2 else r1[p].at[m, :, :, pos[d2], s1v]
        cps = [pltpu.make_async_copy(mine, stage.at[slot, 0, :, :, :, cols], xsem.at[2 + slot, 0])]
        for j in range(1, RING):
            cps.append(pltpu.make_async_copy(r2[p].at[m, rel(pos[d2], j), :, :, s1v], stage.at[slot, j, :, :, :, cols],
                                             xsem.at[2 + slot, j]))
        return cps

    def combine(m, p):
        d1, d2, d3 = PARTS[p]
        n_e = 8 * RING
        r = lax.broadcasted_iota(jnp.int32, (n_e, T), 0)
        e = (r % 2) * 64 + COEF[d3] * ((r // 2) % RING) + COEF[d2] * ((pos[d2] + r // 8) % RING) + COEF[d1] * pos[d1]
        cps = stage_in(m, p, 0, 0)
        for cp in cps:
            cp.start()
        for k in range(RING):
            s1v = rel(pos[d1], k)
            nxt = None
            if k + 1 < RING:
                nxt = stage_in(m, p, k + 1, (k + 1) % 2)
                for cp in nxt:
                    cp.start()
            hit, g = hits(n_e, e, mi[p, pos[d2], s1v, m], mg[p, s1v, m])
            mask = spread(ranks(hit), n_e)
            for cp in cps:
                cp.wait()
            cps = nxt
            rows = stage[k % 2, :, :, :, :, 0:COLS[p]].reshape(n_e * CAP, COLS[p])
            acc = jnp.zeros((T, COLS[p]), F32)
            rest_g = g
            for _ in range(3):
                piece = rest_g.astype(BF).astype(F32)
                rest_g = rest_g - piece
                wt = jnp.where(mask, jnp.broadcast_to(piece[:, None, :], (n_e, CAP, T)), 0.0)
                wt = wt.reshape(n_e * CAP, T).astype(BF)
                acc = acc + lax.dot_general(wt, rows, (((0,), (0,)), ((), ())), preferred_element_type=F32)
            part_acc[p][k] = acc

    r3 = {}

    def r3_one(m, p):
        dim = PARTS[p][0]
        half = T // 2
        a = send(part_acc[p].at[2, pl.ds(0, half)], q1[p].at[m, 0], nb(dim, 1), S.take(), R.take())
        b = send(part_acc[p].at[2, pl.ds(half, half)], q1[p].at[m, 1], nb(dim, -1), S.take(), R.take())
        r3[m, p] = [a, b]

    def r3_two(m, p):
        dim = PARTS[p][0]
        half = T // 2
        a, b = r3[m, p]
        a.wait_recv()
        part_acc[p][1, 0:half] = part_acc[p][1, 0:half] + q1[p][m, 0]
        a2 = send(part_acc[p].at[1], q2[p].at[m, 0], nb(dim, 1), S.take(), R.take())
        b.wait_recv()
        part_acc[p][3, half:T] = part_acc[p][3, half:T] + q1[p][m, 1]
        b2 = send(part_acc[p].at[3], q2[p].at[m, 1], nb(dim, -1), S.take(), R.take())
        r3[m, p] += [a2, b2]

    def r3_end(m, p):
        for cp in r3[m, p][2:]:
            cp.wait_recv()
        cols = slice(offs[p], offs[p] + COLS[p])
        acc = part_acc[p][0] + q2[p][m, 0] + q2[p][m, 1]
        y_ref[m, :, cols] = (h_ref[m, :, cols].astype(F32) + acc).astype(BF)
        for cp in r3[m, p]:
            cp.wait_send()
            del pending[id(cp)]

    dispatch(0)
    p_forward(0)
    dispatch(1)
    p_wait(0)
    for cp in wload:
        cp.wait()
    expert(0, 0, 4)
    p_forward(1)
    expert(0, 4, 8)
    r1_start(0)
    p_wait(1)
    expert(1, 0, 4)
    r1_forward(0)
    expert(1, 4, 8)
    r1_start(1)
    r2_start(0)
    r1_forward(1)
    r2_forward(0)
    r2_start(1)
    for p in P3:
        r2_wait(0, p)
        combine(0, p)
        r3_one(0, p)
    r2_forward(1)
    for p in P3:
        r3_two(0, p)
    for p in P3:
        r3_end(0, p)
    for p in P3:
        r2_wait(1, p)
        combine(1, p)
        r3_one(1, p)
    for p in P3:
        r3_two(1, p)
    for p in P3:
        r3_end(1, p)
    for cp in list(pending.values()):
        cp.wait_send()
    if S.n > nsem or R.n > nsem:
        raise ValueError(f"{S.n} {R.n}")


NSEM = 260


def moe(z, h, idx, gates, w1, w3, w2, cap):
    _, T, D = z.shape
    FF = w1.shape[-1]
    TOP = idx.shape[1]
    COLS = widths(D)
    dims = (T, D, FF, cap, TOP, COLS)
    hbm = []
    for lead in ((2, 2, 4, 4, 4), (2, 2, 4, 4, 4), (2, 2, 4, 4), (2, 4, 2, 4, 4), (2, 2, 4, 4),
                 (2, 4, 4, 2, 4), (2, 2, 2, 2, 4)):
        for p in range(3):
            hbm.append(jax.ShapeDtypeStruct(lead + (cap, COLS[p]), BF))
    V = pltpu.VMEM
    scratch = [V((2, 4, 4, T, COLS[p]), BF) for p in range(3)]
    scratch += [V((8, 4, 4, cap, COLS[p]), BF) for p in range(3)]
    scratch += [V((3, 4, 4, 2, TOP, T), jnp.int32), V((3, 4, 2, TOP, T), F32)]
    scratch += [V((4, 4, cap, COLS[p]), BF) for p in range(3)]
    scratch += [V((D, FF), BF), V((D, FF), BF), V((FF, D), BF), V((2, 4, 4, cap, D), BF), V((2, 4, 4, cap, D), BF)]
    scratch += [V((2, 4, 4, 2, cap, max(COLS)), BF)]
    scratch += [V((4, T, COLS[p]), F32) for p in range(3)]
    scratch += [V((2, 2, T // 2, COLS[p]), F32) for p in range(3)]
    scratch += [V((2, 2, T, COLS[p]), F32) for p in range(3)]
    scratch += [V((16, 8, T), F32)]
    DMA = pltpu.SemaphoreType.DMA
    scratch += [DMA((NSEM,)), DMA((NSEM,)), DMA((4, 4)), DMA((2, 3)), DMA((18,))]
    any_spec = pl.BlockSpec(memory_space=pl.ANY)
    vm = pl.BlockSpec(memory_space=pltpu.VMEM)
    out = pl.pallas_call(
        functools.partial(moe_kernel, dims, NSEM),
        out_shape=[jax.ShapeDtypeStruct((2, T, D), BF)] + hbm,
        in_specs=[any_spec, vm, vm, vm, any_spec, any_spec, any_spec],
        out_specs=[vm] + [any_spec] * len(hbm),
        scratch_shapes=scratch,
        compiler_params=pltpu.CompilerParams(collective_id=0, has_side_effects=True, vmem_limit_bytes=VMEM_LIMIT),
    )(z, h, idx, gates, w1, w3, w2)
    return out[0]


def rms(v, g):
    vf = v.astype(jnp.float32)
    return (vf * lax.rsqrt(jnp.mean(vf * vf, axis=-1, keepdims=True) + 1e-6) * g).astype(jnp.bfloat16)


def attention(x, wq, wk, wv, wo, g):
    ns, seq, d = x.shape
    nh = wq.shape[1] // HEAD
    xf = x.reshape(ns * seq, d)
    u = rms(xf, g)

    def proj(w):
        a = jnp.dot(u, w, preferred_element_type=jnp.float32).astype(jnp.bfloat16)
        return a.reshape(ns, seq, nh, HEAD)

    q, k, v = proj(wq), proj(wk), proj(wv)
    causal = jnp.arange(seq)[:, None] >= jnp.arange(seq)[None, :]
    s = jnp.einsum("bqhe,bkhe->bhqk", q, k, preferred_element_type=jnp.float32) * HEAD ** -0.5
    s = jnp.where(causal, s, -1e30)
    p = jax.nn.softmax(s, axis=-1).astype(jnp.bfloat16)
    o = jnp.einsum("bhqk,bkhe->bqhe", p, v, preferred_element_type=jnp.float32).astype(jnp.bfloat16)
    o = o.reshape(ns * seq, nh * HEAD)
    a = jnp.dot(o, wo, preferred_element_type=jnp.float32)
    return (xf.astype(jnp.float32) + a).astype(jnp.bfloat16)


def capacity(t, top, n_exp):
    return ((top * ((2 * t + n_exp - 1) // n_exp) + 7) // 8) * 8


def solution(mesh):
    ep_axes = ("row", "col")
    tok_axes = ("dp", "row", "col")
    ep = mesh.shape["row"] * mesh.shape["col"]

    def local(x, idx, gates, wq, wk, wv, wo, gattn, gmoe, w1, w3, w2):
        seq, d = x.shape[2:]
        top = idx.shape[-1]
        cap = capacity(seq, top, ep)
        h = attention(x[:, 0], wq, wk, wv, wo, gattn)
        z = rms(h, gmoe)
        y = moe(z.reshape(2, seq, d), h.reshape(2, seq, d), jnp.swapaxes(idx[:, 0], 1, 2),
                jnp.swapaxes(gates[:, 0], 1, 2), w1, w3, w2, cap)
        return y[:, None]

    tok_spec = P(None, tok_axes)
    exp_spec = P(ep_axes)
    return jax.shard_map(local, mesh=mesh,
                         in_specs=(tok_spec, tok_spec, tok_spec, P(), P(), P(), P(), P(), P(), exp_spec, exp_spec, exp_spec),
                         out_specs=tok_spec, check_vma=False)
```

```python
import functools

import jax
import jax.numpy as jnp
from jax import lax
from jax.experimental import pallas as pl
from jax.experimental.pallas import tpu as pltpu
from jax.sharding import PartitionSpec as P

HEAD = 128
VMEM_LIMIT = 67_000_000
HEADS_PER_STEP = 2
ORDER = (
    "mt1", "a1_02", "a1_00", "a1_01", "mt2", "a1_11", "a1_10", "a2_00", "a2_02", "mt3", "a2_10", "a2_01", "a2_11",
    "mt4", "a1_12", "a3_02", "a3_00", "a3_11", "a2_12", "a3_10", "a3_01", "tab", "a4_02", "a4_00", "a3_12", "bd_02",
    "a4_01", "a4_10", "ps_02", "a4_11", "bd_00", "a4_12", "bd_01", "ps_00", "ps_01", "bd_11", "pf_02", "pf_01",
    "bd_10", "ps_11", "pf_00", "bd_12", "ps_12", "ps_10", "E0_0", "E0_1", "pf_10", "E0_2", "pf_11", "E0_3", "E0_4",
    "pf_12", "E0_5", "E0_6", "E0_7", "q1_01", "q1_02", "q1_00", "E1_0", "E1_1", "E1_2", "E1_3", "qf_01", "E1_4",
    "E1_5", "qf_02", "qf_00", "E1_6", "E1_7", "q1_11", "q1_10", "q1_12", "q2_02", "qf_10", "qf_11", "q2_01", "qf_12",
    "q2_10", "qg_10", "qg_02", "q2_12", "qg_01", "q2_11", "ca_02", "q2_00", "qg_00", "qg_12", "ca_10", "qg_11",
    "cb_02", "cb_10", "r3_02", "ca_01", "cb_01", "ca_11", "cb_11", "ca_12", "ca_00", "r3_01", "r3_10", "cb_12",
    "fin_02", "r3_12", "cb_00", "r3_00", "r3_11", "fin_10", "fin_01", "fin_12", "fin_11", "fin_00",
)


MESH = pl.DeviceIdType.MESH
BF = jnp.bfloat16
F32 = jnp.float32
RING = 4
CORES = 2
COEF = {"z": 16, "y": 4, "x": 1}
PARTS = (("x", "y", "z"), ("y", "z", "x"), ("z", "x", "y"))
TILES = CORES * RING


def widths(d):
    lanes = d // 128
    base = lanes // 3
    return (base * 128, base * 128, (lanes - 2 * base) * 128)


class Sems:
    def __init__(self):
        self.n = 0

    def take(self, k=1):
        self.n += k
        return self.n - k


def moe_kernel(dims, nsem, z_hbm, h_ref, idx_ref, gate_ref, w1_hbm, w3_hbm, w2_hbm,
               y_ref, *rest):
    T, D, FF, CAP, TOP, COLS = dims
    it = iter(rest)
    recv = [next(it) for _ in range(3)]
    outp = [next(it) for _ in range(3)]
    ptr = [next(it) for _ in range(3)]
    r1 = [next(it) for _ in range(3)]
    r1t = [next(it) for _ in range(3)]
    r2 = [next(it) for _ in range(3)]
    r2t = [next(it) for _ in range(3)]
    ag = [next(it) for _ in range(3)]
    mi = next(it)
    mg = next(it)
    lst = [next(it) for _ in range(3)]
    w1, w3, w2, xbuf, obuf = (next(it) for _ in range(5))
    stage = next(it)
    part_acc = [next(it) for _ in range(3)]
    q1 = [next(it) for _ in range(3)]
    q2 = [next(it) for _ in range(3)]
    drank = [next(it) for _ in range(3)]
    crank = [next(it) for _ in range(3)]
    cgate = [next(it) for _ in range(3)]
    ssem, rsem = next(it), next(it)
    xsem, osem, lsem, csem = next(it), next(it), next(it), next(it)

    c = lax.axis_index("row")
    q = lax.axis_index("col")
    pos = {"z": q // 16, "y": (q // 4) % 4, "x": q % 4}
    S, R = Sems(), Sems()
    pending = {}
    offs = (0, COLS[0], COLS[0] + COLS[1])

    def rel(v, s):
        return (v + s + RING) % RING

    def nb(dim, s, core=None):
        v = dict(pos)
        v[dim] = rel(v[dim], s)
        return {"row": c if core is None else core, "col": v["z"] * 16 + v["y"] * 4 + v["x"]}

    def make(src, dst, dev, si, ri):
        return pltpu.make_async_remote_copy(src_ref=src, dst_ref=dst, send_sem=ssem.at[si], recv_sem=rsem.at[ri],
                                            device_id=dev, device_id_type=MESH)

    def send(src, dst, dev, si, ri):
        cp = make(src, dst, dev, si, ri)
        cp.start()
        pending[id(cp)] = cp
        return cp

    def wait_in(ref, ri, dev):
        pltpu.make_async_remote_copy(src_ref=ref, dst_ref=ref, send_sem=ssem.at[0], recv_sem=rsem.at[ri],
                                     device_id=dev, device_id_type=MESH).wait_recv()

    barrier = pltpu.get_barrier_semaphore()
    friends = [nb(d, s, core) for d in "xyz" for s in (1, -1) for core in (c, 1 - c)]
    friends.append({"row": 1 - c, "col": q})
    for f in friends:
        pl.semaphore_signal(barrier, inc=1, device_id=f, device_id_type=MESH)
    wload = []
    for i, (a, b) in enumerate(((w1_hbm, w1), (w3_hbm, w3), (w2_hbm, w2))):
        cp = pltpu.make_async_copy(a.at[0], b, lsem.at[i])
        cp.start()
        wload.append(cp)
    own = {}
    for m in range(2):
        for p, (d1, d2, d3) in enumerate(PARTS):
            cp = pltpu.make_async_copy(z_hbm.at[m, :, pl.ds(offs[p], COLS[p])], ag[p].at[m, pos[d2], pos[d1]],
                                       lsem.at[3 + m * 3 + p])
            cp.start()
            own[m, p] = cp
    for p, (d1, d2, d3) in enumerate(PARTS):
        mi[p, pos[d2], pos[d1]] = idx_ref[...]
        mg[p, pos[d1]] = gate_ref[...]
    pl.semaphore_wait(barrier, len(friends))

    def ring1(dim, block):
        me = pos[dim]
        a = send(block(me, None), block(me, None), nb(dim, 1), S.take(), R.take())
        b = send(block(me, None), block(me, None), nb(dim, -1), S.take(), R.take())
        return a, b

    def ring2(dim, block, ab):
        me = pos[dim]
        ab[0].wait_recv()
        a = send(block(rel(me, -1), 0), block(rel(me, -1), 0), nb(dim, 1), S.take(), R.take())
        ab[1].wait_recv()
        b = send(block(rel(me, 1), 1), block(rel(me, 1), 1), nb(dim, -1), S.take(), R.take())
        return a, b

    def ring3(ab):
        ab[0].wait_recv()
        ab[1].wait_recv()

    def blk1(m, p):
        d2 = PARTS[p][1]

        def f(i, half):
            if half is None:
                return ag[p].at[m, pos[d2], i]
            return ag[p].at[m, pos[d2], i, pl.ds(half * (T // 2), T // 2)]
        return f

    def blk2(m, p):
        def f(i, half):
            if half is None:
                return ag[p].at[m, i]
            return ag[p].at[m, i, pl.ds(half * 2, 2)]
        return f

    def mi1(p):
        d2 = PARTS[p][1]

        def f(i, half):
            if half is None:
                return mi.at[p, pos[d2], i]
            return mi.at[p, pos[d2], i, half]
        return f

    def mg1(p):
        def f(i, half):
            if half is None:
                return mg.at[p, i]
            return mg.at[p, i, half]
        return f

    def mi2(p):
        def f(i, half):
            if half is None:
                return mi.at[p, i]
            return mi.at[p, i, pl.ds(half * 2, 2)]
        return f

    P3 = range(3)
    s1, asends = {}, {}

    def a_one(m, p):
        own[m, p].wait()
        s1[m, p] = ring1(PARTS[p][0], blk1(m, p))
        asends[m, p] = list(s1[m, p])

    def a_two(m, p):
        s1[m, p] = ring2(PARTS[p][0], blk1(m, p), s1[m, p])
        asends[m, p] += s1[m, p]

    def a_three(m, p):
        ring3(s1[m, p])
        s1[m, p] = ring1(PARTS[p][1], blk2(m, p))
        asends[m, p] += s1[m, p]

    def a_four(m, p):
        s1[m, p] = ring2(PARTS[p][1], blk2(m, p), s1[m, p])
        asends[m, p] += s1[m, p]

    before = (lax.broadcasted_iota(jnp.int32, (T, T), 0) < lax.broadcasted_iota(jnp.int32, (T, T), 1)).astype(BF)

    def hits(rows, e, idx, gate):
        hit = jnp.zeros((rows, T), F32)
        g = jnp.zeros((rows, T), F32)
        for j in range(TOP):
            eq = jnp.broadcast_to(idx[j:j + 1, :], (rows, T)) == e
            hit = jnp.where(eq, 1.0, hit)
            if gate is not None:
                g = jnp.where(eq, jnp.broadcast_to(gate[j:j + 1, :], (rows, T)), g)
        return hit, g

    def ranks(hit):
        cum = jnp.dot(hit.astype(BF), before, preferred_element_type=F32)
        return jnp.where(hit > 0.0, cum, -1.0)

    def spread(rank, rows):
        slot = lax.broadcasted_iota(jnp.int32, (rows, CAP, T), 1).astype(F32)
        return jnp.broadcast_to(rank[:, None, :], (rows, CAP, T)) == slot

    def tables(p):
        d1, d2, d3 = PARTS[p]
        r = lax.broadcasted_iota(jnp.int32, (2 * RING, T), 0)
        e = (r % 2) * 64 + COEF[d3] * ((pos[d3] + r // 2) % RING) + COEF[d2] * pos[d2] + COEF[d1] * pos[d1]

        def one(i, _):
            drank[p][i], _g = hits(2 * RING, e, mi[p, (i // 4) % 4, i % 4, i // 16], None)
            return 0

        lax.fori_loop(0, 32, one, 0)
        drank[p][...] = ranks(drank[p][...].reshape(32 * 8, T)).reshape(32, 8, T)
        n_e = 8 * RING
        r = lax.broadcasted_iota(jnp.int32, (n_e, T), 0)
        e = (r % 2) * 64 + COEF[d3] * ((r // 2) % RING) + COEF[d2] * ((pos[d2] + r // 8) % RING) + COEF[d1] * pos[d1]

        def two(i, _):
            s1v = (pos[d1] + i % 4) % RING
            hit, g = hits(n_e, e, mi[p, pos[d2], s1v, i // 4], mg[p, s1v, i // 4])
            crank[p][i] = ranks(hit)
            cgate[p][i] = g
            return 0

        lax.fori_loop(0, 8, two, 0)

    def build(m, p):
        for cp in asends.pop((m, p)):
            cp.wait_send()
            del pending[id(cp)]

        def one(s, _):
            sel = jnp.where(spread(drank[p][m * 16 + s], 8), 1.0, 0.0).reshape(8 * CAP, T).astype(BF)
            rows = jnp.dot(sel, ag[p][m, s // 4, s % 4], preferred_element_type=F32)
            ag[p][m, s // 4, s % 4] = rows.astype(BF)
            return 0

        lax.fori_loop(0, 16, one, 0)

    def plane(ref, p, core, t):
        if p == 0:
            return ref.at[core, t]
        if p == 1:
            return ref.at[core, :, :, t]
        return ref.at[core, t]

    def x_start(p, src, dst, transit):
        dim = PARTS[p][2]
        me = pos[dim]
        st = {}
        st["t"] = (send(src(2, 0), transit.at[0], nb(dim, 1), S.take(), R.take()),
                   send(src(2, 1), transit.at[1], nb(dim, -1), S.take(), R.take()))
        st["l"], st["r"], st["o"], st["d"] = R.take(2), R.take(2), R.take(2), R.take()
        st["f"] = (S.take(), S.take())
        for core in range(2):
            send(src(1, core), dst(me, c), nb(dim, 1, core), S.take(), st["l"] + c)
            send(src(3, core), dst(me, c), nb(dim, -1, core), S.take(), st["r"] + c)
        send(src(0, 1 - c), dst(me, c), {"row": 1 - c, "col": q}, S.take(), st["d"])
        return st

    def x_onward(p, dst, transit, st):
        dim = PARTS[p][2]
        me = pos[dim]
        return (make(transit.at[0], dst(rel(me, -1), c), nb(dim, 1, 0), st["f"][0], st["o"] + c),
                make(transit.at[1], dst(rel(me, 1), c), nb(dim, -1, 1), st["f"][1], st["o"] + c))

    def x_forward(p, dst, transit, st):
        for got, cp in zip(st["t"], x_onward(p, dst, transit, st)):
            got.wait_recv()
            cp.start()

    def x_wait(p, dst, transit, st):
        dim = PARTS[p][2]
        me = pos[dim]
        for core in range(2):
            wait_in(dst(rel(me, -1), core), st["l"] + core, nb(dim, -1, core))
            wait_in(dst(rel(me, 1), core), st["r"] + core, nb(dim, 1, core))
            wait_in(dst(rel(me, 2), core), st["o"] + core, nb(dim, 1, core))
        wait_in(dst(me, 1 - c), st["d"], {"row": 1 - c, "col": q})
        for cp in x_onward(p, dst, transit, st):
            cp.wait_send()

    def p_src(m, p):
        return lambda k, core: ag[p].at[m, :, :, pl.ds((2 * k + core) * CAP, CAP)]

    def p_dst(m, p):
        return lambda d3v, core: plane(recv[p].at[m], p, core, d3v)

    def r_src(m, p):
        return lambda k, core: plane(outp[p].at[m], p, core, rel(pos[PARTS[p][2]], k))

    def r_dst(m, p):
        return lambda d3v, core: r1[p].at[m, d3v, core]

    pst, loc = {}, {}

    def p_start(m, p):
        pst[m, p] = x_start(p, p_src(m, p), p_dst(m, p), ptr[p].at[m])
        cp = pltpu.make_async_copy(p_src(m, p)(0, c), p_dst(m, p)(pos[PARTS[p][2]], c), lsem.at[9 + m * 3 + p])
        cp.start()
        loc[m, p] = cp

    def p_forward(m, p):
        x_forward(p, p_dst(m, p), ptr[p].at[m], pst[m, p])

    def p_wait(m):
        for p in P3:
            x_wait(p, p_dst(m, p), ptr[p].at[m], pst[m, p])
            loc.pop((m, p)).wait()

    rows_t = RING * RING * CAP

    def tile_of(refs, m, i, p):
        return refs[p].at[m, i // 4, :, :, i % 4] if p == 2 else refs[p].at[m, i // 4, i % 4]

    def xload(m, i, slot):
        return [pltpu.make_async_copy(tile_of(recv, m, i, p), xbuf.at[slot, :, :, :, pl.ds(offs[p], COLS[p])],
                                      xsem.at[slot, p]) for p in P3]

    def ostore(m, i, slot):
        return [pltpu.make_async_copy(obuf.at[slot, :, :, :, pl.ds(offs[p], COLS[p])], tile_of(outp, m, i, p),
                                      osem.at[slot, p]) for p in P3]

    def expert(m, events):
        for cp in xload(m, 0, 0):
            cp.start()

        def tile(i, _):
            slot = i % 2

            @pl.when(i + 1 < TILES)
            def _():
                for cp in xload(m, i + 1, (i + 1) % 2):
                    cp.start()

            for at, todo in events.items():
                @pl.when(i == at)
                def _():
                    for f in todo:
                        f()

            for cp in xload(m, i, slot):
                cp.wait()

            @pl.when(i >= 2)
            def _():
                for cp in ostore(m, i - 2, slot):
                    cp.wait()

            xt = xbuf[slot].reshape(rows_t, D)
            h1 = jnp.dot(xt, w1[...], preferred_element_type=F32)
            h3 = jnp.dot(xt, w3[...], preferred_element_type=F32)
            act = (jax.nn.silu(h1) * h3).astype(BF)
            o = jnp.dot(act, w2[...], preferred_element_type=F32).astype(BF)
            obuf[slot] = o.reshape(RING, RING, CAP, D)
            for cp in ostore(m, i, slot):
                cp.start()
            return 0

        lax.fori_loop(0, TILES, tile, 0)
        for i in (TILES - 2, TILES - 1):
            for cp in ostore(m, i, i % 2):
                cp.wait()

    rst = {}

    def r1_load(m, p):
        return pltpu.make_async_copy(r_src(m, p)(0, c), lst[p], lsem.at[15 + p])

    def r1_store(m, p):
        return pltpu.make_async_copy(lst[p], r_dst(m, p)(pos[PARTS[p][2]], c), lsem.at[18 + p])

    def r1_start(m, p):
        if m == 1:
            r1_store(0, p).wait()
        rst[m, p] = x_start(p, r_src(m, p), r_dst(m, p), r1t[p].at[m])
        r1_load(m, p).start()

    def r1_forward(m, p):
        x_forward(p, r_dst(m, p), r1t[p].at[m], rst[m, p])
        r1_load(m, p).wait()
        r1_store(m, p).start()

    r2st = {}

    def r2_start(m, p):
        x_wait(p, r_dst(m, p), r1t[p].at[m], rst[m, p])
        if m == 1:
            r1_store(1, p).wait()
        dim = PARTS[p][1]
        me = pos[dim]
        src = r1[p].at[m]
        st = {}
        st["t"] = (send(src.at[pl.ds(0, 2), :, rel(me, 2)], r2t[p].at[m, 0], nb(dim, 1), S.take(), R.take()),
                   send(src.at[pl.ds(2, 2), :, rel(me, 2)], r2t[p].at[m, 1], nb(dim, -1), S.take(), R.take()))
        st["n"] = (send(src.at[:, :, rel(me, 1)], r2[p].at[m, me], nb(dim, 1), S.take(), R.take()),
                   send(src.at[:, :, rel(me, -1)], r2[p].at[m, me], nb(dim, -1), S.take(), R.take()))
        r2st[m, p] = st

    def r2_forward(m, p):
        dim = PARTS[p][1]
        me = pos[dim]
        st = r2st[m, p]
        st["t"][0].wait_recv()
        a = send(r2t[p].at[m, 0], r2[p].at[m, rel(me, -1), pl.ds(0, 2)], nb(dim, 1), S.take(), R.take())
        st["t"][1].wait_recv()
        b = send(r2t[p].at[m, 1], r2[p].at[m, rel(me, 1), pl.ds(2, 2)], nb(dim, -1), S.take(), R.take())
        st["f"] = (a, b)

    def r2_wait(m, p):
        st = r2st[m, p]
        for cp in st["n"] + st["f"]:
            cp.wait_recv()

    def stage_in(m, p, k, slot):
        d1, d2, d3 = PARTS[p]
        s1v = (pos[d1] + k) % RING
        cols = pl.ds(0, COLS[p])
        cps = [pltpu.make_async_copy(r1[p].at[m, :, :, pos[d2], s1v], stage.at[slot, 0, :, :, :, cols],
                                     csem.at[slot, 0])]
        for j in range(1, RING):
            cps.append(pltpu.make_async_copy(r2[p].at[m, rel(pos[d2], j), :, :, s1v], stage.at[slot, j, :, :, :, cols],
                                             csem.at[slot, j]))
        return cps

    def combine(m, p, lo, hi):
        n_e = 8 * RING
        slots = 2 * p
        k_of = lambda i: (2 - i + RING) % RING
        if lo == 0:
            for cp in stage_in(m, p, k_of(0), slots):
                cp.start()

        def one(i, _):
            k = k_of(i)
            slot = slots + i % 2

            @pl.when(i + 1 < RING)
            def _():
                for cp in stage_in(m, p, k_of(i + 1), slots + (i + 1) % 2):
                    cp.start()

            for cp in stage_in(m, p, k, slot):
                cp.wait()
            mask = spread(crank[p][m * 4 + k], n_e)
            rest_g = cgate[p][m * 4 + k]
            rows = stage[slot, :, :, :, :, 0:COLS[p]].reshape(n_e * CAP, COLS[p])
            acc = jnp.zeros((T, COLS[p]), F32)
            for _ in range(3):
                piece = rest_g.astype(BF).astype(F32)
                rest_g = rest_g - piece
                wt = jnp.where(mask, jnp.broadcast_to(piece[:, None, :], (n_e, CAP, T)), 0.0)
                wt = wt.reshape(n_e * CAP, T).astype(BF)
                acc = acc + lax.dot_general(wt, rows, (((0,), (0,)), ((), ())), preferred_element_type=F32)
            part_acc[p][m, k] = acc
            return 0

        lax.fori_loop(lo, hi, one, 0)

    r3 = {}

    def r3_one(m, p):
        dim = PARTS[p][0]
        half = T // 2
        a = send(part_acc[p].at[m, 2, pl.ds(0, half)], q1[p].at[m, 0], nb(dim, 1), S.take(), R.take())
        b = send(part_acc[p].at[m, 2, pl.ds(half, half)], q1[p].at[m, 1], nb(dim, -1), S.take(), R.take())
        r3[m, p] = [a, b]

    def r3_two(m, p):
        dim = PARTS[p][0]
        half = T // 2
        a, b = r3[m, p]
        a.wait_recv()
        part_acc[p][m, 1, 0:half] = part_acc[p][m, 1, 0:half] + q1[p][m, 0]
        a2 = send(part_acc[p].at[m, 1], q2[p].at[m, 0], nb(dim, 1), S.take(), R.take())
        b.wait_recv()
        part_acc[p][m, 3, half:T] = part_acc[p][m, 3, half:T] + q1[p][m, 1]
        b2 = send(part_acc[p].at[m, 3], q2[p].at[m, 1], nb(dim, -1), S.take(), R.take())
        r3[m, p] += [a2, b2]

    def r3_end(m, p):
        for cp in r3[m, p][2:]:
            cp.wait_recv()
        cols = slice(offs[p], offs[p] + COLS[p])
        acc = part_acc[p][m, 0] + q2[p][m, 0] + q2[p][m, 1]
        y_ref[m, :, cols] = (h_ref[m, :, cols].astype(F32) + acc).astype(BF)

    meta = {}

    def meta_one():
        meta["i"] = [ring1(PARTS[p][0], mi1(p)) for p in P3]
        meta["g"] = [ring1(PARTS[p][0], mg1(p)) for p in P3]

    def meta_two():
        meta["i"] = [ring2(PARTS[p][0], mi1(p), meta["i"][p]) for p in P3]
        meta["g"] = [ring2(PARTS[p][0], mg1(p), meta["g"][p]) for p in P3]

    def meta_three():
        for p in P3:
            ring3(meta["i"][p])
        meta["i"] = [ring1(PARTS[p][1], mi2(p)) for p in P3]

    def meta_four():
        meta["i"] = [ring2(PARTS[p][1], mi2(p), meta["i"][p]) for p in P3]

    def meta_five():
        for p in P3:
            ring3(meta["i"][p])
            ring3(meta["g"][p])
            tables(p)

    def slots_in(m, p):
        ring3(s1[m, p])
        build(m, p)

    def sums_one(m, p):
        r2_wait(m, p)
        combine(m, p, 0, 1)
        r3_one(m, p)

    def sums_two(m, p):
        combine(m, p, 1, RING)

    step = {"mt1": meta_one, "mt2": meta_two, "mt3": meta_three, "mt4": meta_four, "tab": meta_five,
            "a1": a_one, "a2": a_two, "a3": a_three, "a4": a_four, "bd": slots_in, "ps": p_start, "pf": p_forward,
            "q1": r1_start, "qf": r1_forward, "q2": r2_start, "qg": r2_forward,
            "ca": sums_one, "cb": sums_two, "r3": r3_two, "fin": r3_end}

    def do(name):
        head, _, tail = name.partition("_")
        step[head](*(int(v) for v in tail))

    queue = list(ORDER)
    while queue:
        name = queue.pop(0)
        if name[0] != "E":
            do(name)
            continue
        m = int(name[1])
        events, at = {}, 1
        while at < TILES:
            nxt = queue.pop(0)
            if nxt[0] == "E":
                at += 1
            else:
                events.setdefault(at, []).append(functools.partial(do, nxt))
        if m == 0:
            for cp in wload:
                cp.wait()
        p_wait(m)
        expert(m, events)
    for cp in list(pending.values()):
        cp.wait_send()
    if S.n > nsem or R.n > nsem:
        raise ValueError(f"{S.n} {R.n}")


NSEM = 252


def moe(z, h, idx, gates, w1, w3, w2, cap):
    _, T, D = z.shape
    FF = w1.shape[-1]
    TOP = idx.shape[1]
    COLS = widths(D)
    dims = (T, D, FF, cap, TOP, COLS)
    hbm = []
    for lead in ((2, 2, 4, 4, 4), (2, 2, 4, 4, 4), (2, 2, 4, 4), (2, 4, 2, 4, 4), (2, 2, 4, 4),
                 (2, 4, 4, 2, 4), (2, 2, 2, 2, 4)):
        for p in range(3):
            hbm.append(jax.ShapeDtypeStruct(lead + (cap, COLS[p]), BF))
    V = pltpu.VMEM
    scratch = [V((2, 4, 4, T, COLS[p]), BF) for p in range(3)]
    scratch += [V((3, 4, 4, 2, TOP, T), jnp.int32), V((3, 4, 2, TOP, T), F32)]
    scratch += [V((4, 4, cap, COLS[p]), BF) for p in range(3)]
    scratch += [V((D, FF), BF), V((D, FF), BF), V((FF, D), BF), V((2, 4, 4, cap, D), BF), V((2, 4, 4, cap, D), BF)]
    scratch += [V((6, 4, 4, 2, cap, max(COLS)), BF)]
    scratch += [V((2, 4, T, COLS[p]), F32) for p in range(3)]
    scratch += [V((2, 2, T // 2, COLS[p]), F32) for p in range(3)]
    scratch += [V((2, 2, T, COLS[p]), F32) for p in range(3)]
    scratch += [V((32, 8, T), F32)] * 3 + [V((8, 32, T), F32)] * 6
    DMA = pltpu.SemaphoreType.DMA
    scratch += [DMA((NSEM,)), DMA((NSEM,)), DMA((2, 3)), DMA((2, 3)), DMA((21,)), DMA((6, 4))]
    any_spec = pl.BlockSpec(memory_space=pl.ANY)
    vm = pl.BlockSpec(memory_space=pltpu.VMEM)
    out = pl.pallas_call(
        functools.partial(moe_kernel, dims, NSEM),
        out_shape=[jax.ShapeDtypeStruct((2, T, D), BF)] + hbm,
        in_specs=[any_spec, vm, vm, vm, any_spec, any_spec, any_spec],
        out_specs=[vm] + [any_spec] * len(hbm),
        scratch_shapes=scratch,
        compiler_params=pltpu.CompilerParams(collective_id=0, has_side_effects=True, vmem_limit_bytes=VMEM_LIMIT),
    )(z, h, idx, gates, w1, w3, w2)
    return out[0]


def attn_kernel(nb, heads, groups, x_ref, ga_ref, gm_ref, wq_ref, wk_ref, wv_ref, wo_ref, h_ref, z_ref,
                u_ref, q_ref, k_ref, v_ref, acc_ref):
    i = pl.program_id(0)
    seq = x_ref.shape[1]
    d = x_ref.shape[2]

    def norm(v, g):
        return (v * lax.rsqrt(jnp.mean(v * v, axis=-1, keepdims=True) + 1e-6) * g).astype(BF)

    @pl.when(i == 0)
    def _():
        u_ref[...] = norm(x_ref[...].reshape(nb * seq, d).astype(F32), ga_ref[...])
        acc_ref[...] = jnp.zeros_like(acc_ref)
        q_ref[...] = jnp.zeros_like(q_ref)
        k_ref[...] = jnp.zeros_like(k_ref)
        v_ref[...] = jnp.zeros_like(v_ref)

    q, k, v = q_ref[...], k_ref[...], v_ref[...]
    causal = (lax.broadcasted_iota(jnp.int32, (seq, seq), 0) >= lax.broadcasted_iota(jnp.int32, (seq, seq), 1))
    u = u_ref[...]
    qn = jnp.dot(u, wq_ref[...], preferred_element_type=F32).astype(BF)
    kn = jnp.dot(u, wk_ref[...], preferred_element_type=F32).astype(BF)
    vn = jnp.dot(u, wv_ref[...], preferred_element_type=F32).astype(BF)
    rows = []
    for b in range(nb):
        cols = []
        for hd in range(heads):
            r, e = slice(b * seq, (b + 1) * seq), slice(hd * HEAD, (hd + 1) * HEAD)
            s = lax.dot_general(q[r, e], k[r, e], (((1,), (1,)), ((), ())), preferred_element_type=F32) * HEAD ** -0.5
            s = jnp.where(causal, s, -1e30)
            p = jnp.exp(s - jnp.max(s, axis=-1, keepdims=True))
            p = (p / jnp.sum(p, axis=-1, keepdims=True)).astype(BF)
            cols.append(jnp.dot(p, v[r, e], preferred_element_type=F32).astype(BF))
        rows.append(jnp.concatenate(cols, axis=1))
    o = jnp.concatenate(rows, axis=0)
    acc_ref[...] += jnp.dot(o, wo_ref[...], preferred_element_type=F32)
    q_ref[...], k_ref[...], v_ref[...] = qn, kn, vn

    @pl.when(i == groups)
    def _():
        h = (x_ref[...].reshape(nb * seq, d).astype(F32) + acc_ref[...]).astype(BF)
        h_ref[...] = h.reshape(nb, seq, d)
        z_ref[...] = norm(h.astype(F32), gm_ref[...]).reshape(nb, seq, d)


def attention(x, wq, wk, wv, wo, gattn, gmoe):
    nb, seq, d = x.shape
    width = wq.shape[1]
    heads = HEADS_PER_STEP
    cols = heads * HEAD
    groups = width // cols
    now = lambda i: jnp.minimum(i, groups - 1)
    whole = pl.BlockSpec((nb, seq, d), lambda i: (0, 0, 0))
    gain = pl.BlockSpec((1, d), lambda i: (0, 0))
    proj = pl.BlockSpec((d, cols), lambda i: (0, now(i)))
    V = pltpu.VMEM
    return pl.pallas_call(
        functools.partial(attn_kernel, nb, heads, groups),
        grid=(groups + 1,),
        out_shape=[jax.ShapeDtypeStruct((nb, seq, d), BF)] * 2,
        in_specs=[whole, gain, gain, proj, proj, proj,
                  pl.BlockSpec((cols, d), lambda i: (jnp.maximum(i - 1, 0), 0))],
        out_specs=[whole, whole],
        scratch_shapes=[V((nb * seq, d), BF)] + [V((nb * seq, cols), BF)] * 3 + [V((nb * seq, d), F32)],
        compiler_params=pltpu.CompilerParams(dimension_semantics=("arbitrary",), vmem_limit_bytes=VMEM_LIMIT),
    )(x, gattn.reshape(1, d), gmoe.reshape(1, d), wq, wk, wv, wo)


def capacity(t, top, n_exp):
    return ((top * ((2 * t + n_exp - 1) // n_exp) + 7) // 8) * 8


def solution(mesh):
    ep_axes = ("row", "col")
    tok_axes = ("dp", "row", "col")
    ep = mesh.shape["row"] * mesh.shape["col"]

    def local(x, idx, gates, wq, wk, wv, wo, gattn, gmoe, w1, w3, w2):
        seq, d = x.shape[2:]
        top = idx.shape[-1]
        cap = capacity(seq, top, ep)
        h, z = attention(x[:, 0], wq, wk, wv, wo, gattn, gmoe)
        y = moe(z, h, jnp.swapaxes(idx[:, 0], 1, 2), jnp.swapaxes(gates[:, 0], 1, 2), w1, w3, w2, cap)
        return y[:, None]

    tok_spec = P(None, tok_axes)
    exp_spec = P(ep_axes)
    return jax.shard_map(local, mesh=mesh,
                         in_specs=(tok_spec, tok_spec, tok_spec, P(), P(), P(), P(), P(), P(), exp_spec, exp_spec, exp_spec),
                         out_specs=tok_spec, check_vma=False)
```

```python
import functools

import jax
import jax.numpy as jnp
from jax import lax
from jax.experimental import pallas as pl
from jax.experimental.pallas import tpu as pltpu
from jax.sharding import PartitionSpec as P

HEAD = 128
VMEM_LIMIT = 67_000_000
HEADS_PER_STEP = 4
ORDER = (
    "mt1", "a1_00", "a1_01", "a1_10", "a1_11", "a1_02", "mt2", "a2_02", "a2_00", "a2_01", "a1_12", "mt3", "a3_02",
    "a3_00", "a3_01", "a2_10", "mt4", "a2_11", "a2_12", "a4_00", "a4_02", "a3_11", "a3_12", "a4_01", "a3_10", "tab",
    "bd_00", "bd_02", "ps_00", "ps_02", "a4_11", "a4_12", "bd_01", "a4_10", "ps_01", "pf_02", "pf_00", "bd_12",
    "bd_11", "pf_01", "ps_11", "bd_10", "ps_10", "ps_12", "E0_0", "E0_1", "E0_2", "E0_3", "pf_11", "pf_10", "E0_4",
    "pf_12", "E0_5", "E0_6", "E0_7", "q1_01", "q1_02", "q1_00", "E1_0", "E1_1", "E1_2", "E1_3", "E1_4", "qf_00",
    "qf_01", "qf_02", "E1_5", "E1_6", "E1_7", "q1_11", "q1_12", "q1_10", "q2_02", "qf_10", "q2_01", "qf_12", "q2_10",
    "qf_11", "qg_01", "qg_02", "q2_12", "qg_10", "q2_11", "ca_02", "q2_00", "cb_02", "qg_00", "ca_01", "qg_12",
    "qg_11", "ca_10", "r3_02", "cb_01", "cb_10", "ca_11", "cb_11", "ca_12", "ca_00", "r3_01", "r3_10", "cb_12",
    "r3_12", "cb_00", "r3_11", "r3_00", "fin_02", "fin_10", "fin_01", "fin_12", "fin_11", "fin_00",
)


MESH = pl.DeviceIdType.MESH
BF = jnp.bfloat16
F32 = jnp.float32
RING = 4
CORES = 2
MICRO = 2
COEF = {"z": 16, "y": 4, "x": 1}
PARTS = (("x", "y", "z"), ("y", "z", "x"), ("z", "x", "y"))
TILES = CORES * RING


def widths(d):
    lanes = d // 128
    base = lanes // 3
    return (base * 128, base * 128, (lanes - 2 * base) * 128)


class Sems:
    def __init__(self):
        self.n = 0

    def take(self, k=1):
        self.n += k
        return self.n - k


def moe_kernel(dims, nsem, z_hbm, h_ref, idx_ref, gate_ref, w1_hbm, w3_hbm, w2_hbm,
               y_ref, *rest):
    T, D, FF, CAP, TOP, COLS = dims
    it = iter(rest)
    recv = [next(it) for _ in range(3)]
    outp = [next(it) for _ in range(3)]
    ptr = [next(it) for _ in range(3)]
    r1 = [next(it) for _ in range(3)]
    r1t = [next(it) for _ in range(3)]
    r2 = [next(it) for _ in range(3)]
    r2t = [next(it) for _ in range(3)]
    ag = [next(it) for _ in range(3)]
    mi = next(it)
    mg = next(it)
    lst = [next(it) for _ in range(3)]
    w1, w3, w2, xbuf, obuf = (next(it) for _ in range(5))
    stage = next(it)
    part_acc = [next(it) for _ in range(3)]
    q1 = [next(it) for _ in range(3)]
    q2 = [next(it) for _ in range(3)]
    drank = [next(it) for _ in range(3)]
    crank = [next(it) for _ in range(3)]
    cgate = [next(it) for _ in range(3)]
    ssem, rsem = next(it), next(it)
    xsem, osem, lsem, csem = next(it), next(it), next(it), next(it)

    c = lax.axis_index("row")
    q = lax.axis_index("col")
    pos = {"z": q // 16, "y": (q // 4) % 4, "x": q % 4}
    S, R = Sems(), Sems()
    unsent = []
    offs = (0, COLS[0], COLS[0] + COLS[1])

    def rel(v, s):
        return (v + s + RING) % RING

    def nb(dim, s, core=None):
        v = dict(pos)
        v[dim] = rel(v[dim], s)
        return {"row": c if core is None else core, "col": v["z"] * 16 + v["y"] * 4 + v["x"]}

    def make(src, dst, dev, si, ri):
        return pltpu.make_async_remote_copy(src_ref=src, dst_ref=dst, send_sem=ssem.at[si], recv_sem=rsem.at[ri],
                                            device_id=dev, device_id_type=MESH)

    def send(src, dst, dev, si, ri):
        make(src, dst, dev, si, ri).start()

    def wait_in(ref, ri):
        make(ref, ref, nb("x", 1), 0, ri).wait_recv()

    def wait_out(ref, si):
        make(ref, ref, nb("x", 1), si, 0).wait_send()

    barrier = pltpu.get_barrier_semaphore()
    friends = [nb(d, s, core) for d in "xyz" for s in (1, -1) for core in (c, 1 - c)]
    friends.append({"row": 1 - c, "col": q})
    for f in friends:
        pl.semaphore_signal(barrier, inc=1, device_id=f, device_id_type=MESH)
    wload = []
    for i, (a, b) in enumerate(((w1_hbm, w1), (w3_hbm, w3), (w2_hbm, w2))):
        cp = pltpu.make_async_copy(a.at[0], b, lsem.at[i])
        cp.start()
        wload.append(cp)
    own = {}
    for m in range(2):
        for p, (d1, d2, d3) in enumerate(PARTS):
            cp = pltpu.make_async_copy(z_hbm.at[m, :, pl.ds(offs[p], COLS[p])], ag[p].at[m, pos[d2], pos[d1]],
                                       lsem.at[3 + m * 3 + p])
            cp.start()
            own[m, p] = cp
    for p, (d1, d2, d3) in enumerate(PARTS):
        mi[p, pos[d2], pos[d1]] = idx_ref[...]
        mg[p, pos[d1]] = gate_ref[...]
    pl.semaphore_wait(barrier, len(friends))

    def ring1(dim, block):
        me = pos[dim]
        g = (S.take(), R.take(), R.take(), R.take())
        send(block(me, None), block(me, None), nb(dim, 1), g[0], g[1])
        send(block(me, None), block(me, None), nb(dim, -1), g[0], g[2])
        return g

    def ring2(dim, block, g):
        left, right = rel(pos[dim], -1), rel(pos[dim], 1)
        wait_in(block(left, None), g[1])
        send(block(left, 0), block(left, 0), nb(dim, 1), g[0], g[3])
        wait_in(block(right, None), g[2])
        send(block(right, 1), block(right, 1), nb(dim, -1), g[0], g[3])

    def ring3(dim, block, g):
        wait_in(block(rel(pos[dim], 2), None), g[3])

    def blk1(m, p):
        d2 = PARTS[p][1]

        def f(i, half):
            if half is None:
                return ag[p].at[m, pos[d2], i]
            return ag[p].at[m, pos[d2], i, pl.ds(half * (T // 2), T // 2)]
        return f

    def blk2(m, p):
        def f(i, half):
            if half is None:
                return ag[p].at[m, i]
            return ag[p].at[m, i, pl.ds(half * 2, 2)]
        return f

    def mi1(p):
        d2 = PARTS[p][1]

        def f(i, half):
            if half is None:
                return mi.at[p, pos[d2], i]
            return mi.at[p, pos[d2], i, half]
        return f

    def mg1(p):
        def f(i, half):
            if half is None:
                return mg.at[p, i]
            return mg.at[p, i, half]
        return f

    def mi2(p):
        def f(i, half):
            if half is None:
                return mi.at[p, i]
            return mi.at[p, i, pl.ds(half * 2, 2)]
        return f

    P3 = range(3)
    g1, g2 = {}, {}

    def a_one(m, p):
        own[m, p].wait()
        g1[m, p] = ring1(PARTS[p][0], blk1(m, p))

    def a_two(m, p):
        ring2(PARTS[p][0], blk1(m, p), g1[m, p])

    def a_three(m, p):
        ring3(PARTS[p][0], blk1(m, p), g1[m, p])
        g2[m, p] = ring1(PARTS[p][1], blk2(m, p))

    def a_four(m, p):
        ring2(PARTS[p][1], blk2(m, p), g2[m, p])

    def a_done(m, p):
        ring3(PARTS[p][1], blk2(m, p), g2[m, p])
        wait_out(ag[p].at[m, pos[PARTS[p][1]], pl.ds(0, 3)], g1[m, p][0])
        wait_out(ag[p].at[m, pl.ds(0, 3)], g2[m, p][0])

    before = (lax.broadcasted_iota(jnp.int32, (T, T), 0) < lax.broadcasted_iota(jnp.int32, (T, T), 1)).astype(BF)

    def hits(rows, e, idx, gate):
        hit = jnp.zeros((rows, T), F32)
        g = jnp.zeros((rows, T), F32)
        for j in range(TOP):
            eq = jnp.broadcast_to(idx[j:j + 1, :], (rows, T)) == e
            hit = jnp.where(eq, 1.0, hit)
            if gate is not None:
                g = jnp.where(eq, jnp.broadcast_to(gate[j:j + 1, :], (rows, T)), g)
        return hit, g

    def ranks(hit):
        cum = jnp.dot(hit.astype(BF), before, preferred_element_type=F32)
        return jnp.where(hit > 0.0, cum, -1.0)

    def spread(rank, rows):
        slot = lax.broadcasted_iota(jnp.int32, (rows, CAP, T), 1).astype(F32)
        return jnp.broadcast_to(rank[:, None, :], (rows, CAP, T)) == slot

    def tables(p):
        d1, d2, d3 = PARTS[p]
        r = lax.broadcasted_iota(jnp.int32, (2 * RING, T), 0)
        e = (r % 2) * 64 + COEF[d3] * ((pos[d3] + r // 2) % RING) + COEF[d2] * pos[d2] + COEF[d1] * pos[d1]

        def one(i, _):
            drank[p][i], _g = hits(2 * RING, e, mi[p, (i // 4) % 4, i % 4, i // 16], None)
            return 0

        lax.fori_loop(0, 32, one, 0)
        drank[p][...] = ranks(drank[p][...].reshape(-1, T)).reshape(drank[p].shape)
        n_e = 8 * RING
        r = lax.broadcasted_iota(jnp.int32, (n_e, T), 0)
        e = (r % 2) * 64 + COEF[d3] * ((r // 2) % RING) + COEF[d2] * ((pos[d2] + r // 8) % RING) + COEF[d1] * pos[d1]

        def two(i, _):
            s1v = (pos[d1] + i % 4) % RING
            hit, g = hits(n_e, e, mi[p, pos[d2], s1v, i // 4], mg[p, s1v, i // 4])
            crank[p][i] = ranks(hit)
            cgate[p][i] = g
            return 0

        lax.fori_loop(0, 8, two, 0)

    def build(m, p):
        def one(s, _):
            sel = jnp.where(spread(drank[p][m * 16 + s], 8), 1.0, 0.0).reshape(8 * CAP, T).astype(BF)
            rows = jnp.dot(sel, ag[p][m, s // 4, s % 4], preferred_element_type=F32)
            ag[p][m, s // 4, s % 4] = rows.astype(BF)
            return 0

        lax.fori_loop(0, 16, one, 0)

    def plane(ref, p, core, t):
        if p == 0:
            return ref.at[core, t]
        if p == 1:
            return ref.at[core, :, :, t]
        return ref.at[core, t]

    def x_start(p, src, dst, transit):
        dim = PARTS[p][2]
        me = pos[dim]
        st = {"s": S.take(), "d": S.take(), "r": R.take(), "t": (R.take(), R.take())}
        send(src(2, 0), transit.at[0], nb(dim, 1), st["s"], st["t"][0])
        send(src(2, 1), transit.at[1], nb(dim, -1), st["s"], st["t"][1])
        for core in range(2):
            send(src(1, core), dst(me, c), nb(dim, 1, core), st["s"], st["r"])
            send(src(3, core), dst(me, c), nb(dim, -1, core), st["s"], st["r"])
        send(src(0, 1 - c), dst(me, c), {"row": 1 - c, "col": q}, st["d"], st["r"])
        return st

    def x_forward(p, dst, transit, st):
        dim = PARTS[p][2]
        me = pos[dim]
        wait_in(transit.at[0], st["t"][0])
        send(transit.at[0], dst(rel(me, -1), c), nb(dim, 1, 0), st["s"], st["r"])
        wait_in(transit.at[1], st["t"][1])
        send(transit.at[1], dst(rel(me, 1), c), nb(dim, -1, 1), st["s"], st["r"])

    def x_wait(p, whole, dst, st):
        wait_in(whole, st["r"])
        unsent.append((whole, st["s"]))
        unsent.append((dst(pos[PARTS[p][2]], c), st["d"]))

    def p_src(m, p):
        return lambda k, core: ag[p].at[m, :, :, pl.ds((2 * k + core) * CAP, CAP)]

    def p_dst(m, p):
        return lambda d3v, core: plane(recv[p].at[m], p, core, d3v)

    def r_src(m, p):
        return lambda k, core: plane(outp[p].at[m], p, core, rel(pos[PARTS[p][2]], k))

    def r_dst(m, p):
        return lambda d3v, core: r1[p].at[m, d3v, core]

    pst = {}

    def p_start(m, p):
        pst[m, p] = x_start(p, p_src(m, p), p_dst(m, p), ptr[p].at[m])
        pltpu.make_async_copy(p_src(m, p)(0, c), p_dst(m, p)(pos[PARTS[p][2]], c), rsem.at[pst[m, p]["r"]]).start()

    def p_forward(m, p):
        x_forward(p, p_dst(m, p), ptr[p].at[m], pst[m, p])

    def p_wait(m):
        for p in P3:
            x_wait(p, recv[p].at[m], p_dst(m, p), pst[m, p])

    rows_t = RING * RING * CAP

    def tile_of(refs, m, i, p):
        return refs[p].at[m, i // 4, :, :, i % 4] if p == 2 else refs[p].at[m, i // 4, i % 4]

    def xload(m, i, slot):
        return [pltpu.make_async_copy(tile_of(recv, m, i, p), xbuf.at[slot, :, :, :, pl.ds(offs[p], COLS[p])],
                                      xsem.at[slot, p]) for p in P3]

    def ostore(m, i, slot):
        return [pltpu.make_async_copy(obuf.at[slot, :, :, :, pl.ds(offs[p], COLS[p])], tile_of(outp, m, i, p),
                                      osem.at[slot, p]) for p in P3]

    def expert(m, events):
        for cp in xload(m, 0, 0):
            cp.start()

        def tile(i, _):
            slot = i % 2

            @pl.when(i + 1 < TILES)
            def _():
                for cp in xload(m, i + 1, (i + 1) % 2):
                    cp.start()

            for at, todo in events.items():
                @pl.when(i == at)
                def _():
                    for f in todo:
                        f()

            for cp in xload(m, i, slot):
                cp.wait()

            @pl.when(i >= 2)
            def _():
                for cp in ostore(m, i - 2, slot):
                    cp.wait()

            xt = xbuf[slot].reshape(rows_t, D)
            h1 = jnp.dot(xt, w1[...], preferred_element_type=F32)
            h3 = jnp.dot(xt, w3[...], preferred_element_type=F32)
            act = (jax.nn.silu(h1) * h3).astype(BF)
            o = jnp.dot(act, w2[...], preferred_element_type=F32).astype(BF)
            obuf[slot] = o.reshape(RING, RING, CAP, D)
            for cp in ostore(m, i, slot):
                cp.start()
            return 0

        lax.fori_loop(0, TILES, tile, 0)
        for i in (TILES - 2, TILES - 1):
            for cp in ostore(m, i, i % 2):
                cp.wait()

    rst = {}

    def r1_load(m, p):
        return pltpu.make_async_copy(r_src(m, p)(0, c), lst[p].at[m], lsem.at[9 + m * 3 + p])

    def r1_store(m, p):
        return pltpu.make_async_copy(lst[p].at[m], r_dst(m, p)(pos[PARTS[p][2]], c), rsem.at[rst[m, p]["r"]])

    def r1_start(m, p):
        rst[m, p] = x_start(p, r_src(m, p), r_dst(m, p), r1t[p].at[m])
        r1_load(m, p).start()

    def r1_forward(m, p):
        x_forward(p, r_dst(m, p), r1t[p].at[m], rst[m, p])
        r1_load(m, p).wait()
        r1_store(m, p).start()

    r2st = {}

    def r2_start(m, p):
        x_wait(p, r1[p].at[m], r_dst(m, p), rst[m, p])
        dim = PARTS[p][1]
        me = pos[dim]
        src = r1[p].at[m]
        st = {"s": S.take(), "r": R.take(), "t": (R.take(), R.take())}
        send(src.at[pl.ds(0, 2), :, rel(me, 2)], r2t[p].at[m, 0], nb(dim, 1), st["s"], st["t"][0])
        send(src.at[pl.ds(2, 2), :, rel(me, 2)], r2t[p].at[m, 1], nb(dim, -1), st["s"], st["t"][1])
        send(src.at[:, :, rel(me, 1)], r2[p].at[m, me], nb(dim, 1), st["s"], st["r"])
        send(src.at[:, :, rel(me, -1)], r2[p].at[m, me], nb(dim, -1), st["s"], st["r"])
        r2st[m, p] = st

    def r2_forward(m, p):
        dim = PARTS[p][1]
        me = pos[dim]
        st = r2st[m, p]
        wait_in(r2t[p].at[m, 0], st["t"][0])
        send(r2t[p].at[m, 0], r2[p].at[m, rel(me, -1), pl.ds(0, 2)], nb(dim, 1), st["s"], st["r"])
        wait_in(r2t[p].at[m, 1], st["t"][1])
        send(r2t[p].at[m, 1], r2[p].at[m, rel(me, 1), pl.ds(2, 2)], nb(dim, -1), st["s"], st["r"])

    def r2_wait(m, p):
        st = r2st[m, p]
        wait_in(r2[p].at[m, pl.ds(0, 3)], st["r"])
        unsent.append((r2[p].at[m], st["s"]))

    def stage_in(m, p, k, slot):
        d1, d2, d3 = PARTS[p]
        s1v = (pos[d1] + k) % RING
        cols = pl.ds(0, COLS[p])
        cps = [pltpu.make_async_copy(r1[p].at[m, :, :, pos[d2], s1v], stage.at[slot, 0, :, :, :, cols],
                                     csem.at[slot, 0])]
        for j in range(1, RING):
            cps.append(pltpu.make_async_copy(r2[p].at[m, rel(pos[d2], j), :, :, s1v], stage.at[slot, j, :, :, :, cols],
                                             csem.at[slot, j]))
        return cps

    def combine(m, p, lo, hi):
        n_e = 8 * RING
        slots = 2 * p
        k_of = lambda i: (2 - i + RING) % RING
        if lo == 0:
            for cp in stage_in(m, p, k_of(0), slots):
                cp.start()

        def one(i, _):
            k = k_of(i)
            slot = slots + i % 2

            @pl.when(i + 1 < RING)
            def _():
                for cp in stage_in(m, p, k_of(i + 1), slots + (i + 1) % 2):
                    cp.start()

            for cp in stage_in(m, p, k, slot):
                cp.wait()
            mask = spread(crank[p][m * 4 + k], n_e)
            rest_g = cgate[p][m * 4 + k]
            rows = stage[slot, :, :, :, :, 0:COLS[p]].reshape(n_e * CAP, COLS[p])
            acc = jnp.zeros((T, COLS[p]), F32)
            for _ in range(3):
                piece = rest_g.astype(BF).astype(F32)
                rest_g = rest_g - piece
                wt = jnp.where(mask, jnp.broadcast_to(piece[:, None, :], (n_e, CAP, T)), 0.0)
                wt = wt.reshape(n_e * CAP, T).astype(BF)
                acc = acc + lax.dot_general(wt, rows, (((0,), (0,)), ((), ())), preferred_element_type=F32)
            part_acc[p][m, k] = acc
            return 0

        lax.fori_loop(lo, hi, one, 0)

    r3 = {}

    def r3_one(m, p):
        dim = PARTS[p][0]
        half = T // 2
        st = {"s": S.take(), "r": R.take(), "t": (R.take(), R.take())}
        send(part_acc[p].at[m, 2, pl.ds(0, half)], q1[p].at[m, 0], nb(dim, 1), st["s"], st["t"][0])
        send(part_acc[p].at[m, 2, pl.ds(half, half)], q1[p].at[m, 1], nb(dim, -1), st["s"], st["t"][1])
        r3[m, p] = st

    def r3_two(m, p):
        dim = PARTS[p][0]
        half = T // 2
        st = r3[m, p]
        wait_in(q1[p].at[m, 0], st["t"][0])
        part_acc[p][m, 1, 0:half] = part_acc[p][m, 1, 0:half] + q1[p][m, 0]
        send(part_acc[p].at[m, 1], q2[p].at[m, 0], nb(dim, 1), st["s"], st["r"])
        wait_in(q1[p].at[m, 1], st["t"][1])
        part_acc[p][m, 3, half:T] = part_acc[p][m, 3, half:T] + q1[p][m, 1]
        send(part_acc[p].at[m, 3], q2[p].at[m, 1], nb(dim, -1), st["s"], st["r"])

    def r3_end(m, p):
        wait_in(q2[p].at[m], r3[m, p]["r"])
        unsent.append((part_acc[p].at[m, pl.ds(0, 3)], r3[m, p]["s"]))
        cols = slice(offs[p], offs[p] + COLS[p])
        acc = part_acc[p][m, 0] + q2[p][m, 0] + q2[p][m, 1]
        y_ref[m, :, cols] = (h_ref[m, :, cols].astype(F32) + acc).astype(BF)

    meta = {}

    def meta_one():
        for p in P3:
            meta[p] = [ring1(PARTS[p][0], mi1(p)), ring1(PARTS[p][0], mg1(p))]

    def meta_two():
        for p in P3:
            ring2(PARTS[p][0], mi1(p), meta[p][0])
            ring2(PARTS[p][0], mg1(p), meta[p][1])

    def meta_three():
        for p in P3:
            ring3(PARTS[p][0], mi1(p), meta[p][0])
            meta[p].append(ring1(PARTS[p][1], mi2(p)))

    def meta_four():
        for p in P3:
            ring2(PARTS[p][1], mi2(p), meta[p][2])

    def meta_five():
        for p in P3:
            ring3(PARTS[p][1], mi2(p), meta[p][2])
            ring3(PARTS[p][0], mg1(p), meta[p][1])
            tables(p)
            unsent.append((mi.at[p, pos[PARTS[p][1]], pl.ds(0, 3)], meta[p][0][0]))
            unsent.append((mg.at[p, pl.ds(0, 3)], meta[p][1][0]))
            unsent.append((mi.at[p, pl.ds(0, 3)], meta[p][2][0]))

    def slots_in(m, p):
        a_done(m, p)
        build(m, p)

    def sums_one(m, p):
        r2_wait(m, p)
        combine(m, p, 0, 1)
        r3_one(m, p)

    def sums_two(m, p):
        combine(m, p, 1, RING)

    step = {"mt1": meta_one, "mt2": meta_two, "mt3": meta_three, "mt4": meta_four, "tab": meta_five,
            "a1": a_one, "a2": a_two, "a3": a_three, "a4": a_four, "bd": slots_in, "ps": p_start, "pf": p_forward,
            "q1": r1_start, "qf": r1_forward, "q2": r2_start, "qg": r2_forward,
            "ca": sums_one, "cb": sums_two, "r3": r3_two, "fin": r3_end}

    def do(name):
        head, _, tail = name.partition("_")
        step[head](*(int(v) for v in tail))

    queue = list(ORDER)
    while queue:
        name = queue.pop(0)
        if name[0] != "E":
            do(name)
            continue
        m = int(name[1])
        events, at = {}, 1
        while at < TILES:
            nxt = queue.pop(0)
            if nxt[0] == "E":
                at += 1
            else:
                events.setdefault(at, []).append(functools.partial(do, nxt))
        if m == 0:
            for cp in wload:
                cp.wait()
        p_wait(m)
        expert(m, events)
    for ref, si in unsent:
        wait_out(ref, si)
    if (S.n, R.n) != nsem:
        raise ValueError(f"{S.n} {R.n}")


NSEM = (57, 135)


def moe(z, h, idx, gates, w1, w3, w2, cap):
    _, T, D = z.shape
    FF = w1.shape[-1]
    TOP = idx.shape[1]
    COLS = widths(D)
    dims = (T, D, FF, cap, TOP, COLS)
    hbm = []
    B, C, R, H, P3 = MICRO, CORES, RING, RING // 2, range(3)
    for lead in ((B, C, R, R, R), (B, C, R, R, R), (B, C, R, R), (B, R, C, R, R), (B, C, R, R),
                 (B, R, R, C, R), (B, C, H, C, R)):
        for p in P3:
            hbm.append(jax.ShapeDtypeStruct(lead + (cap, COLS[p]), BF))
    V = pltpu.VMEM
    scratch = [V((B, R, R, T, COLS[p]), BF) for p in P3]
    scratch += [V((3, R, R, B, TOP, T), jnp.int32), V((3, R, B, TOP, T), F32)]
    scratch += [V((B, R, R, cap, COLS[p]), BF) for p in P3]
    scratch += [V((D, FF), BF), V((D, FF), BF), V((FF, D), BF), V((C, R, R, cap, D), BF), V((C, R, R, cap, D), BF)]
    scratch += [V((3 * C, R, R, C, cap, max(COLS)), BF)]
    scratch += [V((B, R, T, COLS[p]), F32) for p in P3]
    scratch += [V((B, C, T // 2, COLS[p]), F32) for p in P3]
    scratch += [V((B, C, T, COLS[p]), F32) for p in P3]
    scratch += [V((B * R * R, C * R, T), F32) for p in P3]
    scratch += [V((B * R, C * R * R, T), F32) for _ in range(2) for p in P3]
    DMA = pltpu.SemaphoreType.DMA
    scratch += [DMA((NSEM[0],)), DMA((NSEM[1],)), DMA((C, 3)), DMA((C, 3)), DMA((15,)), DMA((3 * C, R))]
    any_spec = pl.BlockSpec(memory_space=pl.ANY)
    vm = pl.BlockSpec(memory_space=pltpu.VMEM)
    out = pl.pallas_call(
        functools.partial(moe_kernel, dims, NSEM),
        out_shape=[jax.ShapeDtypeStruct((2, T, D), BF)] + hbm,
        in_specs=[any_spec, vm, vm, vm, any_spec, any_spec, any_spec],
        out_specs=[vm] + [any_spec] * len(hbm),
        scratch_shapes=scratch,
        compiler_params=pltpu.CompilerParams(collective_id=0, has_side_effects=True, vmem_limit_bytes=VMEM_LIMIT),
    )(z, h, idx, gates, w1, w3, w2)
    return out[0]


def attn_kernel(nb, heads, groups, x_ref, ga_ref, gm_ref, wq_ref, wk_ref, wv_ref, wo_ref, h_ref, z_ref,
                u_ref, acc_ref):
    i = pl.program_id(0)
    seq = x_ref.shape[1]
    d = x_ref.shape[2]

    def norm(v, g):
        return (v * lax.rsqrt(jnp.mean(v * v, axis=-1, keepdims=True) + 1e-6) * g).astype(BF)

    @pl.when(i == 0)
    def _():
        u_ref[...] = norm(x_ref[...].reshape(nb * seq, d).astype(F32), ga_ref[...])
        acc_ref[...] = jnp.zeros_like(acc_ref)

    causal = (lax.broadcasted_iota(jnp.int32, (seq, seq), 0) >= lax.broadcasted_iota(jnp.int32, (seq, seq), 1))
    u = u_ref[...]
    q = jnp.dot(u, wq_ref[...], preferred_element_type=F32).astype(BF)
    k = jnp.dot(u, wk_ref[...], preferred_element_type=F32).astype(BF)
    v = jnp.dot(u, wv_ref[...], preferred_element_type=F32).astype(BF)
    units = [(slice(b * seq, (b + 1) * seq), slice(hd * HEAD, (hd + 1) * HEAD)) for b in range(nb) for hd in range(heads)]
    s = jnp.concatenate([lax.dot_general(q[r, e], k[r, e], (((1,), (1,)), ((), ())), preferred_element_type=F32)[None]
                         for r, e in units], axis=0)
    s = jnp.where(causal[None], s * HEAD ** -0.5, -1e30)
    p = jnp.exp(s - jnp.max(s, axis=-1, keepdims=True))
    p = (p * (1.0 / jnp.sum(p, axis=-1, keepdims=True))).astype(BF)
    ov = [jnp.dot(p[j], v[r, e], preferred_element_type=F32).astype(BF) for j, (r, e) in enumerate(units)]
    o = jnp.concatenate([jnp.concatenate(ov[b * heads:(b + 1) * heads], axis=1) for b in range(nb)], axis=0)
    acc_ref[...] += jnp.dot(o, wo_ref[...], preferred_element_type=F32)

    @pl.when(i == groups - 1)
    def _():
        h = (x_ref[...].reshape(nb * seq, d).astype(F32) + acc_ref[...]).astype(BF)
        h_ref[...] = h.reshape(nb, seq, d)
        z_ref[...] = norm(h.astype(F32), gm_ref[...]).reshape(nb, seq, d)


def attention(x, wq, wk, wv, wo, gattn, gmoe):
    nb, seq, d = x.shape
    width = wq.shape[1]
    heads = HEADS_PER_STEP
    cols = heads * HEAD
    groups = width // cols
    whole = pl.BlockSpec((nb, seq, d), lambda i: (0, 0, 0))
    gain = pl.BlockSpec((1, d), lambda i: (0, 0))
    proj = pl.BlockSpec((d, cols), lambda i: (0, i))
    V = pltpu.VMEM
    return pl.pallas_call(
        functools.partial(attn_kernel, nb, heads, groups),
        grid=(groups,),
        out_shape=[jax.ShapeDtypeStruct((nb, seq, d), BF)] * 2,
        in_specs=[whole, gain, gain, proj, proj, proj,
                  pl.BlockSpec((cols, d), lambda i: (i, 0))],
        out_specs=[whole, whole],
        scratch_shapes=[V((nb * seq, d), BF), V((nb * seq, d), F32)],
        compiler_params=pltpu.CompilerParams(dimension_semantics=("arbitrary",), vmem_limit_bytes=VMEM_LIMIT),
    )(x, gattn.reshape(1, d), gmoe.reshape(1, d), wq, wk, wv, wo)


def capacity(t, top, n_exp):
    return ((top * ((2 * t + n_exp - 1) // n_exp) + 7) // 8) * 8


def solution(mesh):
    ep_axes = ("row", "col")
    tok_axes = ("dp", "row", "col")
    ep = mesh.shape["row"] * mesh.shape["col"]

    def local(x, idx, gates, wq, wk, wv, wo, gattn, gmoe, w1, w3, w2):
        seq, d = x.shape[2:]
        top = idx.shape[-1]
        cap = capacity(seq, top, ep)
        h, z = attention(x[:, 0], wq, wk, wv, wo, gattn, gmoe)
        y = moe(z, h, jnp.swapaxes(idx[:, 0], 1, 2), jnp.swapaxes(gates[:, 0], 1, 2), w1, w3, w2, cap)
        return y[:, None]

    tok_spec = P(None, tok_axes)
    exp_spec = P(ep_axes)
    return jax.shard_map(local, mesh=mesh,
                         in_specs=(tok_spec, tok_spec, tok_spec, P(), P(), P(), P(), P(), P(), exp_spec, exp_spec, exp_spec),
                         out_specs=tok_spec, check_vma=False)
```

```python
import functools

import jax
import jax.numpy as jnp
from jax import lax
from jax.experimental import pallas as pl
from jax.experimental.pallas import tpu as pltpu
from jax.sharding import PartitionSpec as P

HEAD = 128
VMEM_LIMIT = 67_000_000
HEADS_PER_STEP = 8
ORDER = (
    "mt1", "a1_00", "a1_01", "a1_10", "a1_11", "a1_02", "mt2", "a2_02", "a2_00", "a2_01", "a1_12", "mt3", "a3_02",
    "a3_00", "a3_01", "a2_10", "mt4", "a2_11", "a2_12", "a4_00", "a4_02", "a3_11", "a3_12", "a4_01", "a3_10", "tab",
    "bd_00", "bd_02", "ps_00", "ps_02", "a4_11", "a4_12", "bd_01", "a4_10", "ps_01", "pf_02", "pf_00", "bd_12",
    "bd_11", "pf_01", "ps_11", "bd_10", "ps_10", "ps_12", "E0_0", "E0_1", "E0_2", "E0_3", "pf_11", "pf_10", "E0_4",
    "pf_12", "E0_5", "E0_6", "E0_7", "q1_01", "q1_02", "q1_00", "E1_0", "E1_1", "E1_2", "E1_3", "E1_4", "qf_00",
    "qf_01", "qf_02", "E1_5", "E1_6", "E1_7", "q1_11", "q1_12", "q1_10", "q2_02", "qf_10", "q2_01", "qf_12", "q2_10",
    "qf_11", "qg_01", "qg_02", "q2_12", "qg_10", "q2_11", "ca_02", "q2_00", "cb_02", "qg_00", "ca_01", "qg_12",
    "qg_11", "ca_10", "r3_02", "cb_01", "cb_10", "ca_11", "cb_11", "ca_12", "ca_00", "r3_01", "r3_10", "cb_12",
    "r3_12", "cb_00", "r3_11", "r3_00", "fin_02", "fin_10", "fin_01", "fin_12", "fin_11", "fin_00",
)


MESH = pl.DeviceIdType.MESH
BF = jnp.bfloat16
F32 = jnp.float32
RING = 4
CORES = 2
MICRO = 2
COEF = {"z": 16, "y": 4, "x": 1}
PARTS = (("x", "y", "z"), ("y", "z", "x"), ("z", "x", "y"))
TILES = CORES * RING


def widths(d):
    lanes = d // 128
    base = lanes // 3
    return (base * 128, base * 128, (lanes - 2 * base) * 128)


class Sems:
    def __init__(self):
        self.n = 0

    def take(self, k=1):
        self.n += k
        return self.n - k


def moe_kernel(dims, nsem, z_hbm, h_hbm, idx_ref, gate_ref, w1_hbm, w3_hbm, w2_hbm,
               y_hbm, *rest):
    T, D, FF, CAP, TOP, COLS = dims
    it = iter(rest)
    recv = [next(it) for _ in range(3)]
    outp = [next(it) for _ in range(3)]
    ptr = [next(it) for _ in range(3)]
    r1 = [next(it) for _ in range(3)]
    r1t = [next(it) for _ in range(3)]
    r2 = [next(it) for _ in range(3)]
    r2t = [next(it) for _ in range(3)]
    ag = [next(it) for _ in range(3)]
    mi = next(it)
    mg = next(it)
    lst = [next(it) for _ in range(3)]
    w1, w3, w2, xbuf, obuf = (next(it) for _ in range(5))
    stage = next(it)
    part_acc = [next(it) for _ in range(3)]
    q1 = [next(it) for _ in range(3)]
    q2 = [next(it) for _ in range(3)]
    h_ref, y_ref = next(it), next(it)
    drank = [next(it) for _ in range(3)]
    crank = [next(it) for _ in range(3)]
    cgate = [next(it) for _ in range(3)]
    ssem, rsem = next(it), next(it)
    xsem, osem, lsem, csem = next(it), next(it), next(it), next(it)

    c = lax.axis_index("row")
    q = lax.axis_index("col")
    pos = {"z": q // 16, "y": (q // 4) % 4, "x": q % 4}
    S, R = Sems(), Sems()
    unsent = []
    offs = (0, COLS[0], COLS[0] + COLS[1])

    def rel(v, s):
        return (v + s + RING) % RING

    def nb(dim, s, core=None):
        v = dict(pos)
        v[dim] = rel(v[dim], s)
        return {"row": c if core is None else core, "col": v["z"] * 16 + v["y"] * 4 + v["x"]}

    def make(src, dst, dev, si, ri):
        return pltpu.make_async_remote_copy(src_ref=src, dst_ref=dst, send_sem=ssem.at[si], recv_sem=rsem.at[ri],
                                            device_id=dev, device_id_type=MESH)

    def send(src, dst, dev, si, ri):
        make(src, dst, dev, si, ri).start()

    def wait_in(ref, ri):
        make(ref, ref, nb("x", 1), 0, ri).wait_recv()

    def wait_out(ref, si):
        make(ref, ref, nb("x", 1), si, 0).wait_send()

    barrier = pltpu.get_barrier_semaphore()
    friends = [nb(d, s, core) for d in "xyz" for s in (1, -1) for core in (c, 1 - c)]
    friends.append({"row": 1 - c, "col": q})
    for f in friends:
        pl.semaphore_signal(barrier, inc=1, device_id=f, device_id_type=MESH)
    own = {}
    for m in range(2):
        for p, (d1, d2, d3) in enumerate(PARTS):
            cp = pltpu.make_async_copy(z_hbm.at[m, :, pl.ds(offs[p], COLS[p])], ag[p].at[m, pos[d2], pos[d1]],
                                       lsem.at[3 + m * 3 + p])
            cp.start()
            own[m, p] = cp
    wload = []
    for i, (a, b) in enumerate(((w1_hbm, w1), (w3_hbm, w3), (w2_hbm, w2))):
        cp = pltpu.make_async_copy(a.at[0], b, lsem.at[i])
        cp.start()
        wload.append(cp)
    hload = pltpu.make_async_copy(h_hbm, h_ref, lsem.at[15])
    hload.start()
    for p, (d1, d2, d3) in enumerate(PARTS):
        mi[p, pos[d2], pos[d1]] = idx_ref[...]
        mg[p, pos[d1]] = gate_ref[...]
    pl.semaphore_wait(barrier, len(friends))

    def ring1(dim, block):
        me = pos[dim]
        g = (S.take(), R.take(), R.take(), R.take())
        send(block(me, None), block(me, None), nb(dim, 1), g[0], g[1])
        send(block(me, None), block(me, None), nb(dim, -1), g[0], g[2])
        return g

    def ring2(dim, block, g):
        left, right = rel(pos[dim], -1), rel(pos[dim], 1)
        wait_in(block(left, None), g[1])
        send(block(left, 0), block(left, 0), nb(dim, 1), g[0], g[3])
        wait_in(block(right, None), g[2])
        send(block(right, 1), block(right, 1), nb(dim, -1), g[0], g[3])

    def ring3(dim, block, g):
        wait_in(block(rel(pos[dim], 2), None), g[3])

    def blk1(m, p):
        d2 = PARTS[p][1]

        def f(i, half):
            if half is None:
                return ag[p].at[m, pos[d2], i]
            return ag[p].at[m, pos[d2], i, pl.ds(half * (T // 2), T // 2)]
        return f

    def blk2(m, p):
        def f(i, half):
            if half is None:
                return ag[p].at[m, i]
            return ag[p].at[m, i, pl.ds(half * 2, 2)]
        return f

    def mi1(p):
        d2 = PARTS[p][1]

        def f(i, half):
            if half is None:
                return mi.at[p, pos[d2], i]
            return mi.at[p, pos[d2], i, half]
        return f

    def mg1(p):
        def f(i, half):
            if half is None:
                return mg.at[p, i]
            return mg.at[p, i, half]
        return f

    def mi2(p):
        def f(i, half):
            if half is None:
                return mi.at[p, i]
            return mi.at[p, i, pl.ds(half * 2, 2)]
        return f

    P3 = range(3)
    g1, g2 = {}, {}

    def a_one(m, p):
        own[m, p].wait()
        g1[m, p] = ring1(PARTS[p][0], blk1(m, p))

    def a_two(m, p):
        ring2(PARTS[p][0], blk1(m, p), g1[m, p])

    def a_three(m, p):
        ring3(PARTS[p][0], blk1(m, p), g1[m, p])
        g2[m, p] = ring1(PARTS[p][1], blk2(m, p))

    def a_four(m, p):
        ring2(PARTS[p][1], blk2(m, p), g2[m, p])

    def a_done(m, p):
        ring3(PARTS[p][1], blk2(m, p), g2[m, p])
        wait_out(ag[p].at[m, pos[PARTS[p][1]], pl.ds(0, 3)], g1[m, p][0])
        wait_out(ag[p].at[m, pl.ds(0, 3)], g2[m, p][0])

    before = (lax.broadcasted_iota(jnp.int32, (T, T), 0) < lax.broadcasted_iota(jnp.int32, (T, T), 1)).astype(BF)

    def hits(rows, e, idx, gate):
        hit = jnp.zeros((rows, T), F32)
        g = jnp.zeros((rows, T), F32)
        for j in range(TOP):
            eq = jnp.broadcast_to(idx[j:j + 1, :], (rows, T)) == e
            hit = jnp.where(eq, 1.0, hit)
            if gate is not None:
                g = jnp.where(eq, jnp.broadcast_to(gate[j:j + 1, :], (rows, T)), g)
        return hit, g

    def ranks(hit):
        cum = jnp.dot(hit.astype(BF), before, preferred_element_type=F32)
        return jnp.where(hit > 0.0, cum, -1.0)

    def spread(rank, rows):
        slot = lax.broadcasted_iota(jnp.int32, (rows, CAP, T), 1).astype(F32)
        return jnp.broadcast_to(rank[:, None, :], (rows, CAP, T)) == slot

    def tables(p):
        d1, d2, d3 = PARTS[p]
        r = lax.broadcasted_iota(jnp.int32, (2 * RING, T), 0)
        e = (r % 2) * 64 + COEF[d3] * ((pos[d3] + r // 2) % RING) + COEF[d2] * pos[d2] + COEF[d1] * pos[d1]

        def one(i, _):
            drank[p][i], _g = hits(2 * RING, e, mi[p, (i // 4) % 4, i % 4, i // 16], None)
            return 0

        lax.fori_loop(0, 32, one, 0)
        drank[p][...] = ranks(drank[p][...].reshape(-1, T)).reshape(drank[p].shape)
        n_e = 8 * RING
        r = lax.broadcasted_iota(jnp.int32, (n_e, T), 0)
        e = (r % 2) * 64 + COEF[d3] * ((r // 2) % RING) + COEF[d2] * ((pos[d2] + r // 8) % RING) + COEF[d1] * pos[d1]

        def two(i, _):
            s1v = (pos[d1] + i % 4) % RING
            hit, g = hits(n_e, e, mi[p, pos[d2], s1v, i // 4], mg[p, s1v, i // 4])
            crank[p][i] = ranks(hit)
            cgate[p][i] = g
            return 0

        lax.fori_loop(0, 8, two, 0)

    def build(m, p):
        def one(s, _):
            sel = jnp.where(spread(drank[p][m * 16 + s], 8), 1.0, 0.0).reshape(8 * CAP, T).astype(BF)
            rows = jnp.dot(sel, ag[p][m, s // 4, s % 4], preferred_element_type=F32)
            ag[p][m, s // 4, s % 4] = rows.astype(BF)
            return 0

        lax.fori_loop(0, 16, one, 0)

    def plane(ref, p, core, t):
        if p == 0:
            return ref.at[core, t]
        if p == 1:
            return ref.at[core, :, :, t]
        return ref.at[core, t]

    def x_start(p, src, dst, transit):
        dim = PARTS[p][2]
        me = pos[dim]
        st = {"s": S.take(), "d": S.take(), "r": R.take(), "t": (R.take(), R.take())}
        send(src(2, 0), transit.at[0], nb(dim, 1), st["s"], st["t"][0])
        send(src(2, 1), transit.at[1], nb(dim, -1), st["s"], st["t"][1])
        for core in range(2):
            send(src(1, core), dst(me, c), nb(dim, 1, core), st["s"], st["r"])
            send(src(3, core), dst(me, c), nb(dim, -1, core), st["s"], st["r"])
        send(src(0, 1 - c), dst(me, c), {"row": 1 - c, "col": q}, st["d"], st["r"])
        return st

    def x_forward(p, dst, transit, st):
        dim = PARTS[p][2]
        me = pos[dim]
        wait_in(transit.at[0], st["t"][0])
        send(transit.at[0], dst(rel(me, -1), c), nb(dim, 1, 0), st["s"], st["r"])
        wait_in(transit.at[1], st["t"][1])
        send(transit.at[1], dst(rel(me, 1), c), nb(dim, -1, 1), st["s"], st["r"])

    def x_wait(p, whole, dst, st):
        wait_in(whole, st["r"])
        unsent.append((whole, st["s"]))
        unsent.append((dst(pos[PARTS[p][2]], c), st["d"]))

    def p_src(m, p):
        return lambda k, core: ag[p].at[m, :, :, pl.ds((2 * k + core) * CAP, CAP)]

    def p_dst(m, p):
        return lambda d3v, core: plane(recv[p].at[m], p, core, d3v)

    def r_src(m, p):
        return lambda k, core: plane(outp[p].at[m], p, core, rel(pos[PARTS[p][2]], k))

    def r_dst(m, p):
        return lambda d3v, core: r1[p].at[m, d3v, core]

    pst = {}

    def p_start(m, p):
        pst[m, p] = x_start(p, p_src(m, p), p_dst(m, p), ptr[p].at[m])
        pltpu.make_async_copy(p_src(m, p)(0, c), p_dst(m, p)(pos[PARTS[p][2]], c), rsem.at[pst[m, p]["r"]]).start()

    def p_forward(m, p):
        x_forward(p, p_dst(m, p), ptr[p].at[m], pst[m, p])

    def p_wait(m):
        for p in P3:
            x_wait(p, recv[p].at[m], p_dst(m, p), pst[m, p])

    rows_t = RING * RING * CAP

    def tile_of(refs, m, i, p):
        return refs[p].at[m, i // 4, :, :, i % 4] if p == 2 else refs[p].at[m, i // 4, i % 4]

    def xload(m, i, slot):
        return [pltpu.make_async_copy(tile_of(recv, m, i, p), xbuf.at[slot, :, :, :, pl.ds(offs[p], COLS[p])],
                                      xsem.at[slot, p]) for p in P3]

    def ostore(m, i, slot):
        return [pltpu.make_async_copy(obuf.at[slot, :, :, :, pl.ds(offs[p], COLS[p])], tile_of(outp, m, i, p),
                                      osem.at[slot, p]) for p in P3]

    def expert(m, events):
        for cp in xload(m, 0, 0):
            cp.start()

        def tile(i, _):
            slot = i % 2

            @pl.when(i + 1 < TILES)
            def _():
                for cp in xload(m, i + 1, (i + 1) % 2):
                    cp.start()

            for at, todo in events.items():
                @pl.when(i == at)
                def _():
                    for f in todo:
                        f()

            for cp in xload(m, i, slot):
                cp.wait()

            @pl.when(i >= 2)
            def _():
                for cp in ostore(m, i - 2, slot):
                    cp.wait()

            xt = xbuf[slot].reshape(rows_t, D)
            h1 = jnp.dot(xt, w1[...], preferred_element_type=F32)
            h3 = jnp.dot(xt, w3[...], preferred_element_type=F32)
            act = (jax.nn.silu(h1) * h3).astype(BF)
            o = jnp.dot(act, w2[...], preferred_element_type=F32).astype(BF)
            obuf[slot] = o.reshape(RING, RING, CAP, D)
            for cp in ostore(m, i, slot):
                cp.start()
            return 0

        lax.fori_loop(0, TILES, tile, 0)
        for i in (TILES - 2, TILES - 1):
            for cp in ostore(m, i, i % 2):
                cp.wait()

    rst = {}

    def r1_load(m, p):
        return pltpu.make_async_copy(r_src(m, p)(0, c), lst[p].at[m], lsem.at[9 + m * 3 + p])

    def r1_store(m, p):
        return pltpu.make_async_copy(lst[p].at[m], r_dst(m, p)(pos[PARTS[p][2]], c), rsem.at[rst[m, p]["r"]])

    def r1_start(m, p):
        rst[m, p] = x_start(p, r_src(m, p), r_dst(m, p), r1t[p].at[m])
        r1_load(m, p).start()

    def r1_forward(m, p):
        x_forward(p, r_dst(m, p), r1t[p].at[m], rst[m, p])
        r1_load(m, p).wait()
        r1_store(m, p).start()

    r2st = {}

    def r2_start(m, p):
        x_wait(p, r1[p].at[m], r_dst(m, p), rst[m, p])
        dim = PARTS[p][1]
        me = pos[dim]
        src = r1[p].at[m]
        st = {"s": S.take(), "r": R.take(), "t": (R.take(), R.take())}
        send(src.at[pl.ds(0, 2), :, rel(me, 2)], r2t[p].at[m, 0], nb(dim, 1), st["s"], st["t"][0])
        send(src.at[pl.ds(2, 2), :, rel(me, 2)], r2t[p].at[m, 1], nb(dim, -1), st["s"], st["t"][1])
        send(src.at[:, :, rel(me, 1)], r2[p].at[m, me], nb(dim, 1), st["s"], st["r"])
        send(src.at[:, :, rel(me, -1)], r2[p].at[m, me], nb(dim, -1), st["s"], st["r"])
        r2st[m, p] = st

    def r2_forward(m, p):
        dim = PARTS[p][1]
        me = pos[dim]
        st = r2st[m, p]
        wait_in(r2t[p].at[m, 0], st["t"][0])
        send(r2t[p].at[m, 0], r2[p].at[m, rel(me, -1), pl.ds(0, 2)], nb(dim, 1), st["s"], st["r"])
        wait_in(r2t[p].at[m, 1], st["t"][1])
        send(r2t[p].at[m, 1], r2[p].at[m, rel(me, 1), pl.ds(2, 2)], nb(dim, -1), st["s"], st["r"])

    def r2_wait(m, p):
        st = r2st[m, p]
        wait_in(r2[p].at[m, pl.ds(0, 3)], st["r"])
        unsent.append((r2[p].at[m], st["s"]))

    def stage_in(m, p, k, slot):
        d1, d2, d3 = PARTS[p]
        s1v = (pos[d1] + k) % RING
        cols = pl.ds(0, COLS[p])
        cps = [pltpu.make_async_copy(r1[p].at[m, :, :, pos[d2], s1v], stage.at[slot, 0, :, :, :, cols],
                                     csem.at[slot, 0])]
        for j in range(1, RING):
            cps.append(pltpu.make_async_copy(r2[p].at[m, rel(pos[d2], j), :, :, s1v], stage.at[slot, j, :, :, :, cols],
                                             csem.at[slot, j]))
        return cps

    def combine(m, p, lo, hi):
        n_e = 8 * RING
        slots = 2 * p
        k_of = lambda i: (2 - i + RING) % RING
        if lo == 0:
            for cp in stage_in(m, p, k_of(0), slots):
                cp.start()

        def one(i, _):
            k = k_of(i)
            slot = slots + i % 2

            @pl.when(i + 1 < RING)
            def _():
                for cp in stage_in(m, p, k_of(i + 1), slots + (i + 1) % 2):
                    cp.start()

            for cp in stage_in(m, p, k, slot):
                cp.wait()
            mask = spread(crank[p][m * 4 + k], n_e)
            rest_g = cgate[p][m * 4 + k]
            rows = stage[slot, :, :, :, :, 0:COLS[p]].reshape(n_e * CAP, COLS[p])
            acc = jnp.zeros((T, COLS[p]), F32)
            for _ in range(3):
                piece = rest_g.astype(BF).astype(F32)
                rest_g = rest_g - piece
                wt = jnp.where(mask, jnp.broadcast_to(piece[:, None, :], (n_e, CAP, T)), 0.0)
                wt = wt.reshape(n_e * CAP, T).astype(BF)
                acc = acc + lax.dot_general(wt, rows, (((0,), (0,)), ((), ())), preferred_element_type=F32)
            part_acc[p][m, k] = acc
            return 0

        lax.fori_loop(lo, hi, one, 0)

    r3 = {}

    def r3_one(m, p):
        dim = PARTS[p][0]
        half = T // 2
        st = {"s": S.take(), "r": R.take(), "t": (R.take(), R.take())}
        send(part_acc[p].at[m, 2, pl.ds(0, half)], q1[p].at[m, 0], nb(dim, 1), st["s"], st["t"][0])
        send(part_acc[p].at[m, 2, pl.ds(half, half)], q1[p].at[m, 1], nb(dim, -1), st["s"], st["t"][1])
        r3[m, p] = st

    def r3_two(m, p):
        dim = PARTS[p][0]
        half = T // 2
        st = r3[m, p]
        wait_in(q1[p].at[m, 0], st["t"][0])
        part_acc[p][m, 1, 0:half] = part_acc[p][m, 1, 0:half] + q1[p][m, 0]
        send(part_acc[p].at[m, 1], q2[p].at[m, 0], nb(dim, 1), st["s"], st["r"])
        wait_in(q1[p].at[m, 1], st["t"][1])
        part_acc[p][m, 3, half:T] = part_acc[p][m, 3, half:T] + q1[p][m, 1]
        send(part_acc[p].at[m, 3], q2[p].at[m, 1], nb(dim, -1), st["s"], st["r"])

    def y_store(m, p):
        cols = pl.ds(offs[p], COLS[p])
        return pltpu.make_async_copy(y_ref.at[m, :, cols], y_hbm.at[m, :, cols], lsem.at[3 + m * 3 + p])

    def r3_end(m, p):
        wait_in(q2[p].at[m], r3[m, p]["r"])
        unsent.append((part_acc[p].at[m, pl.ds(0, 3)], r3[m, p]["s"]))
        cols = slice(offs[p], offs[p] + COLS[p])
        acc = part_acc[p][m, 0] + q2[p][m, 0] + q2[p][m, 1]
        y_ref[m, :, cols] = (h_ref[m, :, cols].astype(F32) + acc).astype(BF)
        y_store(m, p).start()

    meta = {}

    def meta_one():
        for p in P3:
            meta[p] = [ring1(PARTS[p][0], mi1(p)), ring1(PARTS[p][0], mg1(p))]

    def meta_two():
        for p in P3:
            ring2(PARTS[p][0], mi1(p), meta[p][0])
            ring2(PARTS[p][0], mg1(p), meta[p][1])

    def meta_three():
        for p in P3:
            ring3(PARTS[p][0], mi1(p), meta[p][0])
            meta[p].append(ring1(PARTS[p][1], mi2(p)))

    def meta_four():
        for p in P3:
            ring2(PARTS[p][1], mi2(p), meta[p][2])

    def meta_five():
        for p in P3:
            ring3(PARTS[p][1], mi2(p), meta[p][2])
            ring3(PARTS[p][0], mg1(p), meta[p][1])
            tables(p)
            unsent.append((mi.at[p, pos[PARTS[p][1]], pl.ds(0, 3)], meta[p][0][0]))
            unsent.append((mg.at[p, pl.ds(0, 3)], meta[p][1][0]))
            unsent.append((mi.at[p, pl.ds(0, 3)], meta[p][2][0]))

    def slots_in(m, p):
        a_done(m, p)
        build(m, p)

    def sums_one(m, p):
        r2_wait(m, p)
        combine(m, p, 0, 1)
        r3_one(m, p)

    def sums_two(m, p):
        combine(m, p, 1, RING)

    step = {"mt1": meta_one, "mt2": meta_two, "mt3": meta_three, "mt4": meta_four, "tab": meta_five,
            "a1": a_one, "a2": a_two, "a3": a_three, "a4": a_four, "bd": slots_in, "ps": p_start, "pf": p_forward,
            "q1": r1_start, "qf": r1_forward, "q2": r2_start, "qg": r2_forward,
            "ca": sums_one, "cb": sums_two, "r3": r3_two, "fin": r3_end}

    def do(name):
        head, _, tail = name.partition("_")
        step[head](*(int(v) for v in tail))

    queue = list(ORDER)
    while queue:
        name = queue.pop(0)
        if name[0] != "E":
            do(name)
            continue
        m = int(name[1])
        events, at = {}, 1
        while at < TILES:
            nxt = queue.pop(0)
            if nxt[0] == "E":
                at += 1
            else:
                events.setdefault(at, []).append(functools.partial(do, nxt))
        if m == 0:
            for cp in wload + [hload]:
                cp.wait()
        p_wait(m)
        expert(m, events)
    for ref, si in unsent:
        wait_out(ref, si)
    for m in range(2):
        for p in P3:
            y_store(m, p).wait()
    if (S.n, R.n) != nsem:
        raise ValueError(f"{S.n} {R.n}")


NSEM = (57, 135)


def moe(z, h, idx, gates, w1, w3, w2, cap):
    _, T, D = z.shape
    FF = w1.shape[-1]
    TOP = idx.shape[1]
    COLS = widths(D)
    dims = (T, D, FF, cap, TOP, COLS)
    hbm = []
    B, C, R, H, P3 = MICRO, CORES, RING, RING // 2, range(3)
    for lead in ((B, C, R, R, R), (B, C, R, R, R), (B, C, R, R), (B, R, C, R, R), (B, C, R, R),
                 (B, R, R, C, R), (B, C, H, C, R)):
        for p in P3:
            hbm.append(jax.ShapeDtypeStruct(lead + (cap, COLS[p]), BF))
    V = pltpu.VMEM
    scratch = [V((B, R, R, T, COLS[p]), BF) for p in P3]
    scratch += [V((3, R, R, B, TOP, T), jnp.int32), V((3, R, B, TOP, T), F32)]
    scratch += [V((B, R, R, cap, COLS[p]), BF) for p in P3]
    scratch += [V((D, FF), BF), V((D, FF), BF), V((FF, D), BF), V((C, R, R, cap, D), BF), V((C, R, R, cap, D), BF)]
    scratch += [V((3 * C, R, R, C, cap, max(COLS)), BF)]
    scratch += [V((B, R, T, COLS[p]), F32) for p in P3]
    scratch += [V((B, C, T // 2, COLS[p]), F32) for p in P3]
    scratch += [V((B, C, T, COLS[p]), F32) for p in P3]
    scratch += [V((B, T, D), BF)] * 2
    scratch += [V((B * R * R, C * R, T), F32) for p in P3]
    scratch += [V((B * R, C * R * R, T), F32) for _ in range(2) for p in P3]
    DMA = pltpu.SemaphoreType.DMA
    scratch += [DMA((NSEM[0],)), DMA((NSEM[1],)), DMA((C, 3)), DMA((C, 3)), DMA((16,)), DMA((3 * C, R))]
    any_spec = pl.BlockSpec(memory_space=pl.ANY)
    vm = pl.BlockSpec(memory_space=pltpu.VMEM)
    out = pl.pallas_call(
        functools.partial(moe_kernel, dims, NSEM),
        out_shape=[jax.ShapeDtypeStruct((2, T, D), BF)] + hbm,
        in_specs=[any_spec, any_spec, vm, vm, any_spec, any_spec, any_spec],
        out_specs=[any_spec] * (1 + len(hbm)),
        scratch_shapes=scratch,
        compiler_params=pltpu.CompilerParams(collective_id=0, has_side_effects=True, vmem_limit_bytes=VMEM_LIMIT),
    )(z, h, idx, gates, w1, w3, w2)
    return out[0]


def attn_kernel(nb, heads, groups, x_ref, ga_ref, gm_ref, wq_hbm, wk_hbm, wv_hbm, wo_hbm, h_ref, z_ref,
                wq, wk, wv, wo, u_ref, acc_ref, sem):
    seq, d = x_ref.shape[1:]
    cols = heads * HEAD

    def norm(v, g):
        return (v * lax.rsqrt(jnp.mean(v * v, axis=-1, keepdims=True) + 1e-6) * g).astype(BF)

    def loads(i, slot):
        part = pl.ds(pl.multiple_of(i * cols, HEAD), cols)
        pairs = ((wq_hbm.at[:, part], wq), (wk_hbm.at[:, part], wk), (wv_hbm.at[:, part], wv), (wo_hbm.at[part], wo))
        return [pltpu.make_async_copy(src, dst.at[slot], sem.at[slot, j]) for j, (src, dst) in enumerate(pairs)]

    for cp in loads(0, 0):
        cp.start()
    u_ref[...] = norm(x_ref[...].reshape(nb * seq, d).astype(F32), ga_ref[...])
    acc_ref[...] = jnp.zeros_like(acc_ref)
    causal = (lax.broadcasted_iota(jnp.int32, (seq, seq), 0) >= lax.broadcasted_iota(jnp.int32, (seq, seq), 1))
    units = [(slice(b * seq, (b + 1) * seq), slice(hd * HEAD, (hd + 1) * HEAD)) for b in range(nb) for hd in range(heads)]

    def group(i, _):
        slot = i % 2

        @pl.when(i + 1 < groups)
        def _():
            for cp in loads(i + 1, (i + 1) % 2):
                cp.start()

        here = loads(i, slot)

        def proj(j, w):
            here[j].wait()
            return jnp.dot(u_ref[...], w[slot], preferred_element_type=F32).astype(BF)

        q, k = proj(0, wq), proj(1, wk)
        s = jnp.concatenate([lax.dot_general(q[r, e], k[r, e], (((1,), (1,)), ((), ())), preferred_element_type=F32)[None]
                             for r, e in units], axis=0)
        s = jnp.where(causal[None], s * HEAD ** -0.5, -1e30)
        p = jnp.exp(s - jnp.max(s, axis=-1, keepdims=True))
        p = (p * (1.0 / jnp.sum(p, axis=-1, keepdims=True))).astype(BF)
        v = proj(2, wv)
        ov = [jnp.dot(p[j], v[r, e], preferred_element_type=F32).astype(BF) for j, (r, e) in enumerate(units)]
        o = jnp.concatenate([jnp.concatenate(ov[b * heads:(b + 1) * heads], axis=1) for b in range(nb)], axis=0)
        here[3].wait()
        acc_ref[...] += jnp.dot(o, wo[slot], preferred_element_type=F32)
        return 0

    lax.fori_loop(0, groups, group, 0)
    h = (x_ref[...].reshape(nb * seq, d).astype(F32) + acc_ref[...]).astype(BF)
    h_ref[...] = h.reshape(nb, seq, d)
    z_ref[...] = norm(h.astype(F32), gm_ref[...]).reshape(nb, seq, d)


def attention(x, wq, wk, wv, wo, gattn, gmoe):
    nb, seq, d = x.shape
    width = wq.shape[1]
    heads = HEADS_PER_STEP
    cols = heads * HEAD
    V = pltpu.VMEM
    vm, any_spec = pl.BlockSpec(memory_space=V), pl.BlockSpec(memory_space=pl.ANY)
    return pl.pallas_call(
        functools.partial(attn_kernel, nb, heads, width // cols),
        out_shape=[jax.ShapeDtypeStruct((nb, seq, d), BF)] * 2,
        in_specs=[vm] * 3 + [any_spec] * 4,
        out_specs=[vm, vm],
        scratch_shapes=[V((2, d, cols), BF)] * 3 + [V((2, cols, d), BF), V((nb * seq, d), BF), V((nb * seq, d), F32),
                                                    pltpu.SemaphoreType.DMA((2, 4))],
        compiler_params=pltpu.CompilerParams(vmem_limit_bytes=VMEM_LIMIT),
    )(x, gattn.reshape(1, d), gmoe.reshape(1, d), wq, wk, wv, wo)


def capacity(t, top, n_exp):
    return ((top * ((2 * t + n_exp - 1) // n_exp) + 7) // 8) * 8


def solution(mesh):
    ep_axes = ("row", "col")
    tok_axes = ("dp", "row", "col")
    ep = mesh.shape["row"] * mesh.shape["col"]

    def local(x, idx, gates, wq, wk, wv, wo, gattn, gmoe, w1, w3, w2):
        seq, d = x.shape[2:]
        top = idx.shape[-1]
        cap = capacity(seq, top, ep)
        h, z = attention(x[:, 0], wq, wk, wv, wo, gattn, gmoe)
        y = moe(z, h, jnp.swapaxes(idx[:, 0], 1, 2), jnp.swapaxes(gates[:, 0], 1, 2), w1, w3, w2, cap)
        return y[:, None]

    tok_spec = P(None, tok_axes)
    exp_spec = P(ep_axes)
    return jax.shard_map(local, mesh=mesh,
                         in_specs=(tok_spec, tok_spec, tok_spec, P(), P(), P(), P(), P(), P(), exp_spec, exp_spec, exp_spec),
                         out_specs=tok_spec, check_vma=False)
```

```python
import functools

import jax
import jax.numpy as jnp
from jax import lax
from jax.experimental import pallas as pl
from jax.experimental.pallas import tpu as pltpu
from jax.sharding import PartitionSpec as P

HEAD = 128
VMEM_LIMIT = 67_000_000
HEADS_PER_STEP = 8
ORDER = (
    "mt1", "a1_00", "a1_01", "a1_10", "a1_11", "a1_02", "mt2", "a2_02", "a2_00", "a2_01", "a1_12", "mt3", "a3_02",
    "a3_00", "a3_01", "a2_10", "mt4", "a2_11", "a2_12", "a4_00", "a4_02", "a3_11", "a3_12", "a4_01", "a3_10", "tab",
    "bd_00", "bd_02", "ps_00", "ps_02", "a4_11", "a4_12", "bd_01", "a4_10", "ps_01", "pf_02", "pf_00", "bd_12",
    "bd_11", "pf_01", "ps_11", "bd_10", "ps_10", "ps_12", "E0_0", "E0_1", "E0_2", "E0_3", "pf_11", "pf_10", "E0_4",
    "pf_12", "E0_5", "E0_6", "E0_7", "q1_01", "q1_02", "q1_00", "E1_0", "E1_1", "E1_2", "E1_3", "E1_4", "qf_00",
    "qf_01", "qf_02", "E1_5", "E1_6", "E1_7", "q1_11", "q1_12", "q1_10", "q2_02", "qf_10", "q2_01", "qf_12", "q2_10",
    "qf_11", "qg_01", "qg_02", "q2_12", "qg_10", "q2_11", "ca_02", "q2_00", "cb_02", "qg_00", "ca_01", "qg_12",
    "qg_11", "ca_10", "r3_02", "cb_01", "cb_10", "ca_11", "cb_11", "ca_12", "ca_00", "r3_01", "r3_10", "cb_12",
    "r3_12", "cb_00", "r3_11", "r3_00", "fin_02", "fin_10", "fin_01", "fin_12", "fin_11", "fin_00",
)


MESH = pl.DeviceIdType.MESH
BF = jnp.bfloat16
F32 = jnp.float32
RING = 4
CORES = 2
MICRO = 2
COEF = {"z": 16, "y": 4, "x": 1}
PARTS = (("x", "y", "z"), ("y", "z", "x"), ("z", "x", "y"))
TILES = CORES * RING


def widths(d):
    lanes = d // 128
    base = lanes // 3
    return (base * 128, base * 128, (lanes - 2 * base) * 128)


class Sems:
    def __init__(self):
        self.n = 0

    def take(self, k=1):
        self.n += k
        return self.n - k


def moe_kernel(dims, nsem, z_hbm, h_hbm, idx_ref, gate_ref, w1_hbm, w3_hbm, w2_hbm,
               y_hbm, *rest):
    T, D, FF, CAP, TOP, COLS = dims
    it = iter(rest)
    recv = [next(it) for _ in range(3)]
    outp = [next(it) for _ in range(3)]
    ptr = [next(it) for _ in range(3)]
    r1 = [next(it) for _ in range(3)]
    r1t = [next(it) for _ in range(3)]
    r2 = [next(it) for _ in range(3)]
    r2t = [next(it) for _ in range(3)]
    ag = [next(it) for _ in range(3)]
    mi = next(it)
    mg = next(it)
    lst = [next(it) for _ in range(3)]
    w1, w3, w2, xbuf, obuf = (next(it) for _ in range(5))
    stage = next(it)
    part_acc = [next(it) for _ in range(3)]
    q1 = [next(it) for _ in range(3)]
    q2 = [next(it) for _ in range(3)]
    h_ref, y_ref = next(it), next(it)
    drank = [next(it) for _ in range(3)]
    crank = [next(it) for _ in range(3)]
    cgate = [next(it) for _ in range(3)]
    ssem, rsem = next(it), next(it)
    xsem, osem, lsem, csem = next(it), next(it), next(it), next(it)

    c = lax.axis_index("row")
    q = lax.axis_index("col")
    pos = {"z": q // 16, "y": (q // 4) % 4, "x": q % 4}
    S, R = Sems(), Sems()
    unsent = []
    offs = (0, COLS[0], COLS[0] + COLS[1])

    def rel(v, s):
        return (v + s + RING) % RING

    def nb(dim, s, core=None):
        v = dict(pos)
        v[dim] = rel(v[dim], s)
        return {"row": c if core is None else core, "col": v["z"] * 16 + v["y"] * 4 + v["x"]}

    def make(src, dst, dev, si, ri):
        return pltpu.make_async_remote_copy(src_ref=src, dst_ref=dst, send_sem=ssem.at[si], recv_sem=rsem.at[ri],
                                            device_id=dev, device_id_type=MESH)

    def send(src, dst, dev, si, ri):
        make(src, dst, dev, si, ri).start()

    def wait_in(ref, ri):
        make(ref, ref, nb("x", 1), 0, ri).wait_recv()

    def wait_out(ref, si):
        make(ref, ref, nb("x", 1), si, 0).wait_send()

    barrier = pltpu.get_barrier_semaphore()
    friends = [nb(d, s, core) for d in "xyz" for s in (1, -1) for core in (c, 1 - c)]
    friends.append({"row": 1 - c, "col": q})
    for f in friends:
        pl.semaphore_signal(barrier, inc=1, device_id=f, device_id_type=MESH)
    own = {}
    for m in range(2):
        for p, (d1, d2, d3) in enumerate(PARTS):
            cp = pltpu.make_async_copy(z_hbm.at[m, :, pl.ds(offs[p], COLS[p])], ag[p].at[m, pos[d2], pos[d1]],
                                       lsem.at[3 + m * 3 + p])
            cp.start()
            own[m, p] = cp
    wload = []
    for i, (a, b) in enumerate(((w1_hbm, w1), (w3_hbm, w3), (w2_hbm, w2))):
        cp = pltpu.make_async_copy(a.at[0], b, lsem.at[i])
        cp.start()
        wload.append(cp)
    hload = pltpu.make_async_copy(h_hbm, h_ref, lsem.at[15])
    hload.start()
    for p, (d1, d2, d3) in enumerate(PARTS):
        mi[p, pos[d2], pos[d1]] = idx_ref[...]
        mg[p, pos[d1]] = gate_ref[...]
    pl.semaphore_wait(barrier, len(friends))

    def ring1(dim, block):
        me = pos[dim]
        g = (S.take(), R.take(), R.take(), R.take())
        send(block(me, None), block(me, None), nb(dim, 1), g[0], g[1])
        send(block(me, None), block(me, None), nb(dim, -1), g[0], g[2])
        return g

    def ring2(dim, block, g):
        left, right = rel(pos[dim], -1), rel(pos[dim], 1)
        wait_in(block(left, None), g[1])
        send(block(left, 0), block(left, 0), nb(dim, 1), g[0], g[3])
        wait_in(block(right, None), g[2])
        send(block(right, 1), block(right, 1), nb(dim, -1), g[0], g[3])

    def ring3(dim, block, g):
        wait_in(block(rel(pos[dim], 2), None), g[3])

    def blk1(m, p):
        d2 = PARTS[p][1]

        def f(i, half):
            if half is None:
                return ag[p].at[m, pos[d2], i]
            return ag[p].at[m, pos[d2], i, pl.ds(half * (T // 2), T // 2)]
        return f

    def blk2(m, p):
        def f(i, half):
            if half is None:
                return ag[p].at[m, i]
            return ag[p].at[m, i, pl.ds(half * 2, 2)]
        return f

    def mi1(p):
        d2 = PARTS[p][1]

        def f(i, half):
            if half is None:
                return mi.at[p, pos[d2], i]
            return mi.at[p, pos[d2], i, half]
        return f

    def mg1(p):
        def f(i, half):
            if half is None:
                return mg.at[p, i]
            return mg.at[p, i, half]
        return f

    def mi2(p):
        def f(i, half):
            if half is None:
                return mi.at[p, i]
            return mi.at[p, i, pl.ds(half * 2, 2)]
        return f

    P3 = range(3)
    g1, g2 = {}, {}

    def a_one(m, p):
        own[m, p].wait()
        g1[m, p] = ring1(PARTS[p][0], blk1(m, p))

    def a_two(m, p):
        ring2(PARTS[p][0], blk1(m, p), g1[m, p])

    def a_three(m, p):
        ring3(PARTS[p][0], blk1(m, p), g1[m, p])
        g2[m, p] = ring1(PARTS[p][1], blk2(m, p))

    def a_four(m, p):
        ring2(PARTS[p][1], blk2(m, p), g2[m, p])

    def a_done(m, p):
        ring3(PARTS[p][1], blk2(m, p), g2[m, p])
        wait_out(ag[p].at[m, pos[PARTS[p][1]], pl.ds(0, 3)], g1[m, p][0])
        wait_out(ag[p].at[m, pl.ds(0, 3)], g2[m, p][0])

    before = (lax.broadcasted_iota(jnp.int32, (T, T), 0) < lax.broadcasted_iota(jnp.int32, (T, T), 1)).astype(BF)

    def hits(rows, e, idx, gate):
        hit = jnp.zeros((rows, T), F32)
        g = jnp.zeros((rows, T), F32)
        for j in range(TOP):
            eq = jnp.broadcast_to(idx[j:j + 1, :], (rows, T)) == e
            hit = jnp.where(eq, 1.0, hit)
            if gate is not None:
                g = jnp.where(eq, jnp.broadcast_to(gate[j:j + 1, :], (rows, T)), g)
        return hit, g

    def ranks(hit):
        cum = jnp.dot(hit.astype(BF), before, preferred_element_type=F32)
        return jnp.where(hit > 0.0, cum, -1.0)

    def spread(rank, rows):
        slot = lax.broadcasted_iota(jnp.int32, (rows, CAP, T), 1).astype(F32)
        return jnp.broadcast_to(rank[:, None, :], (rows, CAP, T)) == slot

    def tables(p):
        d1, d2, d3 = PARTS[p]
        r = lax.broadcasted_iota(jnp.int32, (2 * RING, T), 0)
        e = (r % 2) * 64 + COEF[d3] * ((pos[d3] + r // 2) % RING) + COEF[d2] * pos[d2] + COEF[d1] * pos[d1]

        def one(i, _):
            drank[p][i], _g = hits(2 * RING, e, mi[p, (i // 4) % 4, i % 4, i // 16], None)
            return 0

        lax.fori_loop(0, 32, one, 0)
        drank[p][...] = ranks(drank[p][...].reshape(-1, T)).reshape(drank[p].shape)
        n_e = 8 * RING
        r = lax.broadcasted_iota(jnp.int32, (n_e, T), 0)
        e = (r % 2) * 64 + COEF[d3] * ((r // 2) % RING) + COEF[d2] * ((pos[d2] + r // 8) % RING) + COEF[d1] * pos[d1]

        def two(i, _):
            s1v = (pos[d1] + i % 4) % RING
            hit, g = hits(n_e, e, mi[p, pos[d2], s1v, i // 4], mg[p, s1v, i // 4])
            crank[p][i] = ranks(hit)
            cgate[p][i] = g
            return 0

        lax.fori_loop(0, 8, two, 0)

    def build(m, p):
        def one(s, _):
            sel = jnp.where(spread(drank[p][m * 16 + s], 8), 1.0, 0.0).reshape(8 * CAP, T).astype(BF)
            rows = jnp.dot(sel, ag[p][m, s // 4, s % 4], preferred_element_type=F32)
            ag[p][m, s // 4, s % 4] = rows.astype(BF)
            return 0

        lax.fori_loop(0, 16, one, 0)

    def plane(ref, p, core, t):
        if p == 0:
            return ref.at[core, t]
        if p == 1:
            return ref.at[core, :, :, t]
        return ref.at[core, t]

    def x_start(p, src, dst, transit):
        dim = PARTS[p][2]
        me = pos[dim]
        st = {"s": S.take(), "d": S.take(), "r": R.take(), "t": (R.take(), R.take())}
        send(src(2, 0), transit.at[0], nb(dim, 1), st["s"], st["t"][0])
        send(src(2, 1), transit.at[1], nb(dim, -1), st["s"], st["t"][1])
        for core in range(2):
            send(src(1, core), dst(me, c), nb(dim, 1, core), st["s"], st["r"])
            send(src(3, core), dst(me, c), nb(dim, -1, core), st["s"], st["r"])
        send(src(0, 1 - c), dst(me, c), {"row": 1 - c, "col": q}, st["d"], st["r"])
        return st

    def x_forward(p, dst, transit, st):
        dim = PARTS[p][2]
        me = pos[dim]
        wait_in(transit.at[0], st["t"][0])
        send(transit.at[0], dst(rel(me, -1), c), nb(dim, 1, 0), st["s"], st["r"])
        wait_in(transit.at[1], st["t"][1])
        send(transit.at[1], dst(rel(me, 1), c), nb(dim, -1, 1), st["s"], st["r"])

    def x_wait(p, whole, dst, st):
        wait_in(whole, st["r"])
        unsent.append((whole, st["s"]))
        unsent.append((dst(pos[PARTS[p][2]], c), st["d"]))

    def p_src(m, p):
        return lambda k, core: ag[p].at[m, :, :, pl.ds((2 * k + core) * CAP, CAP)]

    def p_dst(m, p):
        return lambda d3v, core: plane(recv[p].at[m], p, core, d3v)

    def r_src(m, p):
        return lambda k, core: plane(outp[p].at[m], p, core, rel(pos[PARTS[p][2]], k))

    def r_dst(m, p):
        return lambda d3v, core: r1[p].at[m, d3v, core]

    pst = {}

    def p_start(m, p):
        pst[m, p] = x_start(p, p_src(m, p), p_dst(m, p), ptr[p].at[m])
        pltpu.make_async_copy(p_src(m, p)(0, c), p_dst(m, p)(pos[PARTS[p][2]], c), rsem.at[pst[m, p]["r"]]).start()

    def p_forward(m, p):
        x_forward(p, p_dst(m, p), ptr[p].at[m], pst[m, p])

    def p_wait(m):
        for p in P3:
            x_wait(p, recv[p].at[m], p_dst(m, p), pst[m, p])

    rows_t = RING * RING * CAP

    def tile_of(refs, m, i, p):
        return refs[p].at[m, i // 4, :, :, i % 4] if p == 2 else refs[p].at[m, i // 4, i % 4]

    def xload(m, i, slot):
        return [pltpu.make_async_copy(tile_of(recv, m, i, p), xbuf.at[slot, :, :, :, pl.ds(offs[p], COLS[p])],
                                      xsem.at[slot, p]) for p in P3]

    def ostore(m, i, slot):
        return [pltpu.make_async_copy(obuf.at[slot, :, :, :, pl.ds(offs[p], COLS[p])], tile_of(outp, m, i, p),
                                      osem.at[slot, p]) for p in P3]

    def expert(m, events):
        for cp in xload(m, 0, 0):
            cp.start()

        def tile(i, _):
            slot = i % 2

            @pl.when(i + 1 < TILES)
            def _():
                for cp in xload(m, i + 1, (i + 1) % 2):
                    cp.start()

            for at, todo in events.items():
                @pl.when(i == at)
                def _():
                    for f in todo:
                        f()

            for cp in xload(m, i, slot):
                cp.wait()

            @pl.when(i >= 2)
            def _():
                for cp in ostore(m, i - 2, slot):
                    cp.wait()

            xt = xbuf[slot].reshape(rows_t, D)
            h1 = jnp.dot(xt, w1[...], preferred_element_type=F32)
            h3 = jnp.dot(xt, w3[...], preferred_element_type=F32)
            act = (jax.nn.silu(h1) * h3).astype(BF)
            o = jnp.dot(act, w2[...], preferred_element_type=F32).astype(BF)
            obuf[slot] = o.reshape(RING, RING, CAP, D)
            for cp in ostore(m, i, slot):
                cp.start()
            return 0

        lax.fori_loop(0, TILES, tile, 0)
        for i in (TILES - 2, TILES - 1):
            for cp in ostore(m, i, i % 2):
                cp.wait()

    rst = {}

    def r1_load(m, p):
        return pltpu.make_async_copy(r_src(m, p)(0, c), lst[p].at[m], lsem.at[9 + m * 3 + p])

    def r1_store(m, p):
        return pltpu.make_async_copy(lst[p].at[m], r_dst(m, p)(pos[PARTS[p][2]], c), rsem.at[rst[m, p]["r"]])

    def r1_start(m, p):
        rst[m, p] = x_start(p, r_src(m, p), r_dst(m, p), r1t[p].at[m])
        r1_load(m, p).start()

    def r1_forward(m, p):
        x_forward(p, r_dst(m, p), r1t[p].at[m], rst[m, p])
        r1_load(m, p).wait()
        r1_store(m, p).start()

    r2st = {}

    def r2_start(m, p):
        x_wait(p, r1[p].at[m], r_dst(m, p), rst[m, p])
        dim = PARTS[p][1]
        me = pos[dim]
        src = r1[p].at[m]
        st = {"s": S.take(), "r": R.take(), "t": (R.take(), R.take())}
        send(src.at[pl.ds(0, 2), :, rel(me, 2)], r2t[p].at[m, 0], nb(dim, 1), st["s"], st["t"][0])
        send(src.at[pl.ds(2, 2), :, rel(me, 2)], r2t[p].at[m, 1], nb(dim, -1), st["s"], st["t"][1])
        send(src.at[:, :, rel(me, 1)], r2[p].at[m, me], nb(dim, 1), st["s"], st["r"])
        send(src.at[:, :, rel(me, -1)], r2[p].at[m, me], nb(dim, -1), st["s"], st["r"])
        r2st[m, p] = st

    def r2_forward(m, p):
        dim = PARTS[p][1]
        me = pos[dim]
        st = r2st[m, p]
        wait_in(r2t[p].at[m, 0], st["t"][0])
        send(r2t[p].at[m, 0], r2[p].at[m, rel(me, -1), pl.ds(0, 2)], nb(dim, 1), st["s"], st["r"])
        wait_in(r2t[p].at[m, 1], st["t"][1])
        send(r2t[p].at[m, 1], r2[p].at[m, rel(me, 1), pl.ds(2, 2)], nb(dim, -1), st["s"], st["r"])

    def r2_wait(m, p):
        st = r2st[m, p]
        wait_in(r2[p].at[m, pl.ds(0, 3)], st["r"])
        unsent.append((r2[p].at[m], st["s"]))

    def stage_in(m, p, k, slot):
        d1, d2, d3 = PARTS[p]
        s1v = (pos[d1] + k) % RING
        cols = pl.ds(0, COLS[p])
        cps = [pltpu.make_async_copy(r1[p].at[m, :, :, pos[d2], s1v], stage.at[slot, 0, :, :, :, cols],
                                     csem.at[slot, 0])]
        for j in range(1, RING):
            cps.append(pltpu.make_async_copy(r2[p].at[m, rel(pos[d2], j), :, :, s1v], stage.at[slot, j, :, :, :, cols],
                                             csem.at[slot, j]))
        return cps

    def combine(m, p, lo, hi):
        n_e = 8 * RING
        slots = 2 * p
        k_of = lambda i: (2 - i + RING) % RING
        if lo == 0:
            for cp in stage_in(m, p, k_of(0), slots):
                cp.start()

        def one(i, _):
            k = k_of(i)
            slot = slots + i % 2

            @pl.when(i + 1 < RING)
            def _():
                for cp in stage_in(m, p, k_of(i + 1), slots + (i + 1) % 2):
                    cp.start()

            for cp in stage_in(m, p, k, slot):
                cp.wait()
            mask = spread(crank[p][m * 4 + k], n_e)
            rest_g = cgate[p][m * 4 + k]
            rows = stage[slot, :, :, :, :, 0:COLS[p]].reshape(n_e * CAP, COLS[p])
            acc = jnp.zeros((T, COLS[p]), F32)
            for _ in range(3):
                piece = rest_g.astype(BF).astype(F32)
                rest_g = rest_g - piece
                wt = jnp.where(mask, jnp.broadcast_to(piece[:, None, :], (n_e, CAP, T)), 0.0)
                wt = wt.reshape(n_e * CAP, T).astype(BF)
                acc = acc + lax.dot_general(wt, rows, (((0,), (0,)), ((), ())), preferred_element_type=F32)
            part_acc[p][m, k] = acc
            return 0

        lax.fori_loop(lo, hi, one, 0)

    r3 = {}

    def r3_one(m, p):
        dim = PARTS[p][0]
        half = T // 2
        st = {"s": S.take(), "r": R.take(), "t": (R.take(), R.take())}
        send(part_acc[p].at[m, 2, pl.ds(0, half)], q1[p].at[m, 0], nb(dim, 1), st["s"], st["t"][0])
        send(part_acc[p].at[m, 2, pl.ds(half, half)], q1[p].at[m, 1], nb(dim, -1), st["s"], st["t"][1])
        r3[m, p] = st

    def r3_two(m, p):
        dim = PARTS[p][0]
        half = T // 2
        st = r3[m, p]
        wait_in(q1[p].at[m, 0], st["t"][0])
        part_acc[p][m, 1, 0:half] = part_acc[p][m, 1, 0:half] + q1[p][m, 0]
        send(part_acc[p].at[m, 1], q2[p].at[m, 0], nb(dim, 1), st["s"], st["r"])
        wait_in(q1[p].at[m, 1], st["t"][1])
        part_acc[p][m, 3, half:T] = part_acc[p][m, 3, half:T] + q1[p][m, 1]
        send(part_acc[p].at[m, 3], q2[p].at[m, 1], nb(dim, -1), st["s"], st["r"])

    def y_store(m, p):
        cols = pl.ds(offs[p], COLS[p])
        return pltpu.make_async_copy(y_ref.at[m, :, cols], y_hbm.at[m, :, cols], lsem.at[3 + m * 3 + p])

    def r3_end(m, p):
        wait_in(q2[p].at[m], r3[m, p]["r"])
        unsent.append((part_acc[p].at[m, pl.ds(0, 3)], r3[m, p]["s"]))
        cols = slice(offs[p], offs[p] + COLS[p])
        acc = part_acc[p][m, 0] + q2[p][m, 0] + q2[p][m, 1]
        y_ref[m, :, cols] = (h_ref[m, :, cols].astype(F32) + acc).astype(BF)
        y_store(m, p).start()

    meta = {}

    def meta_one():
        for p in P3:
            meta[p] = [ring1(PARTS[p][0], mi1(p)), ring1(PARTS[p][0], mg1(p))]

    def meta_two():
        for p in P3:
            ring2(PARTS[p][0], mi1(p), meta[p][0])
            ring2(PARTS[p][0], mg1(p), meta[p][1])

    def meta_three():
        for p in P3:
            ring3(PARTS[p][0], mi1(p), meta[p][0])
            meta[p].append(ring1(PARTS[p][1], mi2(p)))

    def meta_four():
        for p in P3:
            ring2(PARTS[p][1], mi2(p), meta[p][2])

    def meta_five():
        for p in P3:
            ring3(PARTS[p][1], mi2(p), meta[p][2])
            ring3(PARTS[p][0], mg1(p), meta[p][1])
            tables(p)
            unsent.append((mi.at[p, pos[PARTS[p][1]], pl.ds(0, 3)], meta[p][0][0]))
            unsent.append((mg.at[p, pl.ds(0, 3)], meta[p][1][0]))
            unsent.append((mi.at[p, pl.ds(0, 3)], meta[p][2][0]))

    def slots_in(m, p):
        a_done(m, p)
        build(m, p)

    def sums_one(m, p):
        r2_wait(m, p)
        combine(m, p, 0, 1)
        r3_one(m, p)

    def sums_two(m, p):
        combine(m, p, 1, RING)

    step = {"mt1": meta_one, "mt2": meta_two, "mt3": meta_three, "mt4": meta_four, "tab": meta_five,
            "a1": a_one, "a2": a_two, "a3": a_three, "a4": a_four, "bd": slots_in, "ps": p_start, "pf": p_forward,
            "q1": r1_start, "qf": r1_forward, "q2": r2_start, "qg": r2_forward,
            "ca": sums_one, "cb": sums_two, "r3": r3_two, "fin": r3_end}

    def do(name):
        head, _, tail = name.partition("_")
        step[head](*(int(v) for v in tail))

    queue = list(ORDER)
    while queue:
        name = queue.pop(0)
        if name[0] != "E":
            do(name)
            continue
        m = int(name[1])
        events, at = {}, 1
        while at < TILES:
            nxt = queue.pop(0)
            if nxt[0] == "E":
                at += 1
            else:
                events.setdefault(at, []).append(functools.partial(do, nxt))
        if m == 0:
            for cp in wload + [hload]:
                cp.wait()
        p_wait(m)
        expert(m, events)
    for ref, si in unsent:
        wait_out(ref, si)
    for m in range(2):
        for p in P3:
            y_store(m, p).wait()
    if (S.n, R.n) != nsem:
        raise ValueError(f"{S.n} {R.n}")


NSEM = (57, 135)


def moe(z, h, idx, gates, w1, w3, w2, cap):
    _, T, D = z.shape
    FF = w1.shape[-1]
    TOP = idx.shape[1]
    COLS = widths(D)
    dims = (T, D, FF, cap, TOP, COLS)
    hbm = []
    B, C, R, H, P3 = MICRO, CORES, RING, RING // 2, range(3)
    for lead in ((B, C, R, R, R), (B, C, R, R, R), (B, C, R, R), (B, R, C, R, R), (B, C, R, R),
                 (B, R, R, C, R), (B, C, H, C, R)):
        for p in P3:
            hbm.append(jax.ShapeDtypeStruct(lead + (cap, COLS[p]), BF))
    V = pltpu.VMEM
    scratch = [V((B, R, R, T, COLS[p]), BF) for p in P3]
    scratch += [V((3, R, R, B, TOP, T), jnp.int32), V((3, R, B, TOP, T), F32)]
    scratch += [V((B, R, R, cap, COLS[p]), BF) for p in P3]
    scratch += [V((D, FF), BF), V((D, FF), BF), V((FF, D), BF), V((C, R, R, cap, D), BF), V((C, R, R, cap, D), BF)]
    scratch += [V((3 * C, R, R, C, cap, max(COLS)), BF)]
    scratch += [V((B, R, T, COLS[p]), F32) for p in P3]
    scratch += [V((B, C, T // 2, COLS[p]), F32) for p in P3]
    scratch += [V((B, C, T, COLS[p]), F32) for p in P3]
    scratch += [V((B, T, D), BF)] * 2
    scratch += [V((B * R * R, C * R, T), F32) for p in P3]
    scratch += [V((B * R, C * R * R, T), F32) for _ in range(2) for p in P3]
    DMA = pltpu.SemaphoreType.DMA
    scratch += [DMA((NSEM[0],)), DMA((NSEM[1],)), DMA((C, 3)), DMA((C, 3)), DMA((16,)), DMA((3 * C, R))]
    any_spec = pl.BlockSpec(memory_space=pl.ANY)
    vm = pl.BlockSpec(memory_space=pltpu.VMEM)
    out = pl.pallas_call(
        functools.partial(moe_kernel, dims, NSEM),
        out_shape=[jax.ShapeDtypeStruct((2, T, D), BF)] + hbm,
        in_specs=[any_spec, any_spec, vm, vm, any_spec, any_spec, any_spec],
        out_specs=[any_spec] * (1 + len(hbm)),
        scratch_shapes=scratch,
        compiler_params=pltpu.CompilerParams(collective_id=0, has_side_effects=True, vmem_limit_bytes=VMEM_LIMIT),
    )(z, h, idx, gates, w1, w3, w2)
    return settle(out[0])


def settle_kernel(chunks, src, dst, buf, isem, osem):
    rows = src.shape[1] // chunks
    parts = [(m, pl.ds(i * rows, rows)) for m in range(src.shape[0]) for i in range(chunks)]
    ins = [pltpu.make_async_copy(src.at[p], buf.at[p], isem.at[j]) for j, p in enumerate(parts)]
    outs = [pltpu.make_async_copy(buf.at[p], dst.at[p], osem.at[j]) for j, p in enumerate(parts)]
    for cp in ins:
        cp.start()
    for a, b in zip(ins, outs):
        a.wait()
        b.start()
    for cp in outs:
        cp.wait()


def settle(y):
    chunks = 2
    n = y.shape[0] * chunks
    any_spec = pl.BlockSpec(memory_space=pl.ANY)
    return pl.pallas_call(
        functools.partial(settle_kernel, chunks), out_shape=jax.ShapeDtypeStruct(y.shape, y.dtype),
        in_specs=[any_spec], out_specs=any_spec,
        scratch_shapes=[pltpu.VMEM(y.shape, y.dtype), pltpu.SemaphoreType.DMA((n,)), pltpu.SemaphoreType.DMA((n,))],
        compiler_params=pltpu.CompilerParams(vmem_limit_bytes=VMEM_LIMIT),
    )(y)


def attn_kernel(nb, heads, groups, x_ref, ga_ref, gm_ref, wq_hbm, wk_hbm, wv_hbm, wo_hbm, h_ref, z_ref,
                wq, wk, wv, wo, u_ref, acc_ref, sem):
    seq, d = x_ref.shape[1:]
    cols = heads * HEAD

    def norm(v, g):
        return (v * lax.rsqrt(jnp.mean(v * v, axis=-1, keepdims=True) + 1e-6) * g).astype(BF)

    def loads(i, slot):
        part = pl.ds(pl.multiple_of(i * cols, HEAD), cols)
        pairs = ((wq_hbm.at[:, part], wq), (wk_hbm.at[:, part], wk), (wv_hbm.at[:, part], wv), (wo_hbm.at[part], wo))
        return [pltpu.make_async_copy(src, dst.at[slot], sem.at[slot, j]) for j, (src, dst) in enumerate(pairs)]

    for cp in loads(0, 0):
        cp.start()
    u_ref[...] = norm(x_ref[...].reshape(nb * seq, d).astype(F32), ga_ref[...])
    acc_ref[...] = jnp.zeros_like(acc_ref)
    causal = (lax.broadcasted_iota(jnp.int32, (seq, seq), 0) >= lax.broadcasted_iota(jnp.int32, (seq, seq), 1))
    units = [(slice(b * seq, (b + 1) * seq), slice(hd * HEAD, (hd + 1) * HEAD)) for b in range(nb) for hd in range(heads)]

    def group(i, _):
        slot = i % 2

        @pl.when(i + 1 < groups)
        def _():
            for cp in loads(i + 1, (i + 1) % 2):
                cp.start()

        here = loads(i, slot)

        def proj(j, w):
            here[j].wait()
            return jnp.dot(u_ref[...], w[slot], preferred_element_type=F32).astype(BF)

        q, k = proj(0, wq), proj(1, wk)
        s = jnp.concatenate([lax.dot_general(q[r, e], k[r, e], (((1,), (1,)), ((), ())), preferred_element_type=F32)[None]
                             for r, e in units], axis=0)
        s = jnp.where(causal[None], s * HEAD ** -0.5, -1e30)
        p = jnp.exp(s - jnp.max(s, axis=-1, keepdims=True))
        p = (p * (1.0 / jnp.sum(p, axis=-1, keepdims=True))).astype(BF)
        v = proj(2, wv)
        ov = [jnp.dot(p[j], v[r, e], preferred_element_type=F32).astype(BF) for j, (r, e) in enumerate(units)]
        o = jnp.concatenate([jnp.concatenate(ov[b * heads:(b + 1) * heads], axis=1) for b in range(nb)], axis=0)
        here[3].wait()
        acc_ref[...] += jnp.dot(o, wo[slot], preferred_element_type=F32)
        return 0

    lax.fori_loop(0, groups, group, 0)
    h = (x_ref[...].reshape(nb * seq, d).astype(F32) + acc_ref[...]).astype(BF)
    h_ref[...] = h.reshape(nb, seq, d)
    z_ref[...] = norm(h.astype(F32), gm_ref[...]).reshape(nb, seq, d)


def attention(x, wq, wk, wv, wo, gattn, gmoe):
    nb, seq, d = x.shape
    width = wq.shape[1]
    heads = HEADS_PER_STEP
    cols = heads * HEAD
    V = pltpu.VMEM
    vm, any_spec = pl.BlockSpec(memory_space=V), pl.BlockSpec(memory_space=pl.ANY)
    return pl.pallas_call(
        functools.partial(attn_kernel, nb, heads, width // cols),
        out_shape=[jax.ShapeDtypeStruct((nb, seq, d), BF)] * 2,
        in_specs=[vm] * 3 + [any_spec] * 4,
        out_specs=[vm, vm],
        scratch_shapes=[V((2, d, cols), BF)] * 3 + [V((2, cols, d), BF), V((nb * seq, d), BF), V((nb * seq, d), F32),
                                                    pltpu.SemaphoreType.DMA((2, 4))],
        compiler_params=pltpu.CompilerParams(vmem_limit_bytes=VMEM_LIMIT),
    )(x, gattn.reshape(1, d), gmoe.reshape(1, d), wq, wk, wv, wo)


def capacity(t, top, n_exp):
    return ((top * ((2 * t + n_exp - 1) // n_exp) + 7) // 8) * 8


def solution(mesh):
    ep_axes = ("row", "col")
    tok_axes = ("dp", "row", "col")
    ep = mesh.shape["row"] * mesh.shape["col"]

    def local(x, idx, gates, wq, wk, wv, wo, gattn, gmoe, w1, w3, w2):
        seq, d = x.shape[2:]
        top = idx.shape[-1]
        cap = capacity(seq, top, ep)
        h, z = attention(x[:, 0], wq, wk, wv, wo, gattn, gmoe)
        y = moe(z, h, jnp.swapaxes(idx[:, 0], 1, 2), jnp.swapaxes(gates[:, 0], 1, 2), w1, w3, w2, cap)
        return y[:, None]

    tok_spec = P(None, tok_axes)
    exp_spec = P(ep_axes)
    return jax.shard_map(local, mesh=mesh,
                         in_specs=(tok_spec, tok_spec, tok_spec, P(), P(), P(), P(), P(), P(), exp_spec, exp_spec, exp_spec),
                         out_specs=tok_spec, check_vma=False)
```
